32 devices in a mesh: fit: 1 (over z), comp: 4 (over y), pts: 8 (over x, core).
Axes of the slice: x: 4, y: 4, z: 1, core: 2. Of those that a mesh axis runs over, the one named last changes fastest.
The devices are a block of a 4x4x8 slice.
Arguments:
- points: bfloat16 [16384, 512], P(('fit', 'pts'))
- means_init: float32 [4096, 512], P(('fit', 'comp'))
- logw_init: float32 [4096], P(('fit', 'comp'))
- inv_temp: float32 [3], replicated
Outputs:
- output 1: float32 [4096, 512], P(('fit', 'comp'))
- output 2: float32 [4096], P(('fit', 'comp'))
- output 3: float32 [16384], P(('fit', 'pts'))
All inputs are finite; a program needn't handle non-finite values.
Results may differ from the reference program's by a relative error of at most 0.001.
Values are sent between devices in bfloat16 or wider.
A program may use at most 768 MiB of HBM per device.

```python
import jax
import jax.numpy as jnp
from jax import lax

N = 16384
K = 4096
D = 512
SWEEPS = 3
NUM_SRC = 32
ROW_BLOCK = 1024

PRIOR_ALPHA = 1e-3
COUNT_EPS = 1e-6


def setup_inputs(seed: int = 0, part: int = 0) -> dict:
    root_key = jax.random.key(seed)
    part_key = jax.random.fold_in(root_key, part)
    key_cent, key_noise, key_assign, key_mnoise, key_logw = jax.random.split(part_key, 5)
    key_temp = jax.random.fold_in(root_key, 1000003)
    center_std = (2.0 / D ** 0.5) ** 0.5
    centers = center_std * jax.random.normal(key_cent, (NUM_SRC, D), jnp.float32)
    src_id = (jnp.arange(N, dtype=jnp.int32) * NUM_SRC) // N
    points = centers[src_id] + jax.random.normal(key_noise, (N, D), jnp.float32)
    assign = jax.random.randint(key_assign, (K,), 0, NUM_SRC)
    means_init = centers[assign] + 0.8 * jax.random.normal(key_mnoise, (K, D), jnp.float32)
    logw_init = jax.nn.log_softmax(0.5 * jax.random.normal(key_logw, (K,), jnp.float32))
    temp_steps = jax.random.uniform(key_temp, (SWEEPS,), jnp.float32)
    inv_temp = (0.25 + 0.2 * jnp.cumsum(temp_steps)) / D ** 0.5
    return {"points": points.astype(jnp.bfloat16), "means_init": means_init, "logw_init": logw_init, "inv_temp": inv_temp}


def em_sweep(points, mean_vecs, log_w, temp):
    mean_bf = mean_vecs.astype(jnp.bfloat16)
    mean_sq = jnp.sum(mean_vecs * mean_vecs, axis=1)
    row_blocks = points.reshape(N // ROW_BLOCK, ROW_BLOCK, D)

    def scan_body(state_pair, row_blk):
        counts, stat_sums = state_pair
        x_sq = jnp.sum(jnp.square(row_blk.astype(jnp.float32)), axis=1)
        cross_dot = jnp.dot(row_blk, mean_bf.T, preferred_element_type=jnp.float32)
        logits = log_w[None, :] - temp * (x_sq[:, None] - 2.0 * cross_dot + mean_sq[None, :])
        row_top = jnp.max(logits, axis=1)
        exp_total = jnp.sum(jnp.exp(logits - row_top[:, None]), axis=1)
        log_norm = row_top + jnp.log(exp_total)
        resp_prob = jnp.exp(logits - log_norm[:, None])
        counts = counts + jnp.sum(resp_prob, axis=0)
        stat_sums = stat_sums + jnp.dot(resp_prob.astype(jnp.bfloat16).T, row_blk, preferred_element_type=jnp.float32)
        return (counts, stat_sums), log_norm

    init_state = (jnp.zeros((K,), jnp.float32), jnp.zeros((K, D), jnp.float32))
    (counts, stat_sums), log_norm = lax.scan(scan_body, init_state, row_blocks)
    new_means = stat_sums / (counts[:, None] + COUNT_EPS)
    new_logw = jnp.log((counts + PRIOR_ALPHA) / (N + K * PRIOR_ALPHA))
    return new_means, new_logw, log_norm.reshape(N)


def reference(points, means_init, logw_init, inv_temp):
    mean_vecs = means_init
    log_w = logw_init
    log_norm = jnp.zeros((N,), jnp.float32)
    for sweep_idx in range(SWEEPS):
        mean_vecs, log_w, log_norm = em_sweep(points, mean_vecs, log_w, inv_temp[sweep_idx])
    return mean_vecs, log_w, log_norm
```

```python
import functools
import math

import jax
import jax.numpy as jnp
from jax import lax
from jax.experimental import pallas as pl
from jax.experimental.pallas import tpu as pltpu
from jax.sharding import PartitionSpec as P

PRIOR_ALPHA = 1e-3
COUNT_EPS = 1e-6
LOG2E = math.log2(math.e)
LN2 = math.log(2.0)
MESH = pl.DeviceIdType.MESH
CORES = 2
LANES = 128

OPP, RIGHT, LEFT, OWN = range(4)
SHIFT = {OPP: 2, RIGHT: 1, LEFT: 3, OWN: 0}


def em_kernel(
    sweeps, n_total, k_total, n_chips, n_comp,
    beta_ref, x_hbm, mean_hbm, logw_ref,
    mean_out, logw_out, lse_out,
    x_all, xt, hq, e_buf, r_buf, mean_f, mean_b, prm, m_st, s_st, pair_out, pair_in, glob_out, glob_in,
    lse_own, lse_oth, s_buf, rs_in, acc_out, n_out, n_in, row_out, row_in, send_sem, recv_sem, copy_sem,
):
    n_loc, depth = x_all.shape[1], x_all.shape[2]
    kq = mean_f.shape[1]
    kh = kq // 2
    half = n_chips * kq

    p = lax.axis_index("pts")
    y = lax.axis_index("comp")
    chip = lax.div(p, CORES)
    core = p - chip * CORES
    partner = {"pts": chip * CORES + 1 - core}

    def x_peer(d):
        return {"pts": lax.rem(chip + d, n_chips) * CORES + core}

    right, left, opposite = x_peer(1), x_peer(n_chips - 1), x_peer(2)
    y_peers = [{"comp": lax.rem(y + d, n_comp)} for d in range(1, n_comp)]

    barrier = pltpu.get_barrier_semaphore()
    everyone = [partner, right, left, opposite] + y_peers
    for dev in everyone:
        pl.semaphore_signal(barrier, inc=1, device_id=dev, device_id_type=MESH)

    load_x = pltpu.make_async_copy(x_hbm, x_all.at[0], copy_sem.at[4])
    load_x.start()
    load_mean = []
    for b in range(4):
        q = lax.rem(chip + SHIFT[b], n_chips)
        c = pltpu.make_async_copy(
            mean_hbm.at[pl.ds(pl.multiple_of(core * half + q * kq, kq), kq)], mean_f.at[b], copy_sem.at[b]
        )
        c.start()
        load_mean.append(c)

    pending = []

    def send(src, dst, t, idx, dev):
        c = pltpu.make_async_remote_copy(
            src_ref=src, dst_ref=dst, send_sem=send_sem.at[t, idx], recv_sem=recv_sem.at[t, idx],
            device_id=dev, device_id_type=MESH,
        )
        c.start()
        pending.append(c)
        return c

    def drain():
        for c in pending:
            c.wait_send()
        pending.clear()

    eye = lax.broadcasted_iota(jnp.int32, (kq, kq), 0) == lax.broadcasted_iota(jnp.int32, (kq, kq), 1)

    def to_col(row):
        return jnp.sum(jnp.where(eye, jnp.broadcast_to(row, (kq, kq)), 0.0), axis=1, keepdims=True)

    def to_row(col):
        return jnp.sum(jnp.where(eye, jnp.broadcast_to(col, (kq, kq)), 0.0), axis=0, keepdims=True)

    pl.semaphore_wait(barrier, len(everyone))
    x_copy = send(x_hbm, x_all.at[1], 0, 31, partner)

    load_x.wait()
    for b in range(4):
        load_mean[b].wait()
        mf = mean_f[b]
        mean_b[0, b] = mf.astype(jnp.bfloat16)
        q = lax.rem(chip + SHIFT[b], n_chips)
        prm[0, b, 0:1, :] = logw_ref[pl.ds(core * n_chips + q, 1), :] * LOG2E
        prm[0, b, 1:2, :] = to_row(0.5 * jnp.sum(mf * mf, axis=1, keepdims=True))

    tr = min(512, n_loc)

    def prepare(h):
        @pl.loop(0, n_loc // tr)
        def _(c):
            rows = pl.ds(pl.multiple_of(c * tr, tr), tr)
            cols = pl.ds(pl.multiple_of(h * n_loc + c * tr, tr), tr)
            blk = x_all[h, rows, :].T
            xt[:, cols] = blk
            f = blk.astype(jnp.float32)
            hq[:, cols] = 0.5 * jnp.sum(f * f, axis=0, keepdims=True)

    tile = min(256, n_loc)
    unroll = min(4, n_loc // tile)

    def a_phase(t, h, blocks):
        neg_beta2 = beta_ref[t] * (-2.0 * LOG2E)
        lp = [to_col(prm[t, b, 0:1, :]) for b in blocks]
        hm = [to_col(prm[t, b, 1:2, :]) for b in blocks]
        lo, nb = blocks[0], len(blocks)

        @pl.loop(0, n_loc // (tile * unroll))
        def _(c):
            for u in range(unroll):
                cols = pl.ds(pl.multiple_of(h * n_loc + (c * unroll + u) * tile, tile), tile)
                means = mean_b[t, lo:lo + nb].reshape(nb * kq, depth)
                a_all = jnp.dot(means, xt[:, cols], preferred_element_type=jnp.float32)
                hqc = hq[:, cols]
                for i, b in enumerate(blocks):
                    a = a_all[i * kq:(i + 1) * kq]
                    logit = ((hqc - a) + hm[i]) * neg_beta2 + lp[i]
                    m = jnp.max(logit, axis=0, keepdims=True)
                    e = jnp.exp2(logit - m)
                    e_buf[b * kq:(b + 1) * kq, cols] = e
                    m_st[b:b + 1, cols] = m
                    s_st[b:b + 1, cols] = jnp.sum(e, axis=0, keepdims=True)

    def local_pair(h):
        cols = pl.ds(h * n_loc, n_loc)
        ms = [m_st[b:b + 1, cols] for b in range(4)]
        m = jnp.maximum(jnp.maximum(ms[0], ms[1]), jnp.maximum(ms[2], ms[3]))
        s = sum(s_st[b:b + 1, cols] * jnp.exp2(ms[b] - m) for b in range(4))
        return m, s

    def r_phase(h, blocks, lse, accs):
        rt = min(512, n_loc)

        def body(c, acc):
            acc = list(acc)
            cols = pl.ds(pl.multiple_of(h * n_loc + c * rt, rt), rt)
            l2 = lse[:, pl.ds(pl.multiple_of(c * rt, rt), rt)]
            for i, b in enumerate(blocks):
                f = jnp.exp2(m_st[b:b + 1, cols] - l2)
                r = e_buf[b * kq:(b + 1) * kq, cols] * f
                r_buf[b * kq:(b + 1) * kq, cols] = r.astype(jnp.bfloat16)
                for v in range(rt // LANES):
                    acc[i] = acc[i] + r[:, v * LANES:(v + 1) * LANES]
            return tuple(acc)

        return lax.fori_loop(0, n_loc // rt, body, accs)

    zero = jnp.zeros((kq, LANES), jnp.float32)

    for t in range(sweeps):
        last = t == sweeps - 1
        if t == 0:
            prepare(0)
            for pair in ((0, 1), (2, 3)):
                a_phase(t, 0, pair)
            x_copy.wait_recv()
            prepare(1)
            for pair in ((0, 1), (2, 3)):
                a_phase(t, 1, pair)
        else:
            gather[1].wait_recv()
            gather[6].wait_recv()
            a_phase(t, 1, (LEFT,))
            a_phase(t, 0, (LEFT,))
            gather[4].wait_recv()
            gather[7].wait_recv()
            a_phase(t, 1, (RIGHT,))
            a_phase(t, 0, (RIGHT,))
            gather[2].wait_recv()
            gather[5].wait_recv()
            gather[8].wait_recv()
            a_phase(t, 1, (OPP,))
        m, s = local_pair(1)
        pair_out[t, 0:1, :] = m
        pair_out[t, 1:2, :] = s
        pair = send(pair_out.at[t], pair_in.at[t], t, 0, partner)
        if t > 0:
            a_phase(t, 0, (OPP,))
        m, s = local_pair(0)
        pair.wait_recv()
        m1, s1 = pair_in[t, 0:1, :], pair_in[t, 1:2, :]
        top = jnp.maximum(m, m1)
        s = s * jnp.exp2(m - top) + s1 * jnp.exp2(m1 - top)
        glob_out[t, 0:1, :] = top
        glob_out[t, 1:2, :] = s
        across = [
            send(glob_out.at[t], glob_in.at[t, d], t, 1 + d, y_peers[d]) for d in range(n_comp - 1)
        ]
        tops, sums = [top], [s]
        for d in range(n_comp - 1):
            across[d].wait_recv()
            tops.append(glob_in[t, d, 0:1, :])
            sums.append(glob_in[t, d, 1:2, :])
        top = functools.reduce(jnp.maximum, tops)
        total = sum(v * jnp.exp2(w - top) for v, w in zip(sums, tops))
        lse2 = top + jnp.log(total) * LOG2E
        lse_own[t] = lse2
        swap = send(lse_own.at[t], lse_oth.at[t], t, 4, partner)
        if last:
            lse_out[...] = lse2 * LN2

        own_r = lse_own.at[t]
        accs = r_phase(0, (0, 1, 2, 3), own_r, (zero,) * 4)
        swap.wait_recv()
        oth_r = lse_oth.at[t]
        acc_a = r_phase(1, (0, 1), oth_r, accs[:2])
        counts = []

        def stats(lo):
            out = jnp.dot(
                r_buf[lo * kq:(lo + 2) * kq, 0:n_loc], x_all[0], preferred_element_type=jnp.float32
            )
            out += jnp.dot(
                r_buf[lo * kq:(lo + 2) * kq, n_loc:2 * n_loc], x_all[1], preferred_element_type=jnp.float32
            )
            s_buf[t, 2 * lo:2 * lo + 4] = out.reshape(4, kh, depth)

        stats(0)
        scat = [
            send(s_buf.at[t, 2 * OPP], rs_in.at[t, 0], t, 5, right),
            send(s_buf.at[t, 2 * OPP + 1], rs_in.at[t, 1], t, 6, left),
            send(s_buf.at[t, 2 * RIGHT + 1], rs_in.at[t, 2], t, 7, right),
        ]
        acc_b = r_phase(1, (2, 3), oth_r, accs[2:])
        for b, acc in enumerate(tuple(acc_a) + tuple(acc_b)):
            row = to_row(jnp.sum(acc, axis=1, keepdims=True))
            n_out[t, b, 0:1, :] = row
            counts.append(row)
        n_copies = [
            send(n_out.at[t, OPP], n_in.at[t, 0], t, 8, opposite),
            send(n_out.at[t, RIGHT], n_in.at[t, 1], t, 9, right),
            send(n_out.at[t, LEFT], n_in.at[t, 2], t, 10, left),
        ]
        stats(2)
        scat.append(send(s_buf.at[t, 2 * LEFT], rs_in.at[t, 3], t, 11, left))
        scat[0].wait_recv()
        acc_out[t, 0] = s_buf[t, 2 * RIGHT] + rs_in[t, 0]
        scat.append(send(acc_out.at[t, 0], rs_in.at[t, 4], t, 12, right))
        scat[1].wait_recv()
        acc_out[t, 1] = s_buf[t, 2 * LEFT + 1] + rs_in[t, 1]
        scat.append(send(acc_out.at[t, 1], rs_in.at[t, 5], t, 13, left))

        n_row = counts[OWN]
        for d in range(3):
            n_copies[d].wait_recv()
            n_row = n_row + n_in[t, d, 0:1, :]
        n_col = to_col(n_row) + COUNT_EPS
        logw = jnp.log((n_row + PRIOR_ALPHA) / (n_total + k_total * PRIOR_ALPHA))

        scat[3].wait_recv()
        scat[4].wait_recv()
        mean_lo = (s_buf[t, 2 * OWN] + rs_in[t, 3] + rs_in[t, 4]) / n_col[:kh]
        if not last:
            nxt = mean_b.at[t + 1]
            a_rows, b_rows = pl.ds(0, kh), pl.ds(kh, kh)
            mean_b[t + 1, OWN, 0:kh, :] = mean_lo.astype(jnp.bfloat16)
            mine_a, mine_b = nxt.at[OWN, a_rows], nxt.at[OWN, b_rows]
            g0 = send(mine_a, nxt.at[LEFT, a_rows], t, 14, right)
            scat[2].wait_recv()
            scat[5].wait_recv()
            mean_hi = (s_buf[t, 2 * OWN + 1] + rs_in[t, 2] + rs_in[t, 5]) / n_col[kh:]
            mean_b[t + 1, OWN, kh:kq, :] = mean_hi.astype(jnp.bfloat16)
            g3 = send(mine_b, nxt.at[RIGHT, b_rows], t, 17, left)
            g1 = send(mine_b, nxt.at[LEFT, b_rows], t, 15, right)
            g4 = send(mine_a, nxt.at[RIGHT, a_rows], t, 18, left)
            sq = jnp.concatenate(
                [jnp.sum(mean_lo * mean_lo, axis=1, keepdims=True), jnp.sum(mean_hi * mean_hi, axis=1, keepdims=True)], axis=0
            )
            prm[t + 1, OWN, 0:1, :] = logw * LOG2E
            prm[t + 1, OWN, 1:2, :] = to_row(0.5 * sq)
            src = prm.at[t + 1, OWN]
            g6 = send(src, prm.at[t + 1, LEFT], t, 20, right)
            g7 = send(src, prm.at[t + 1, RIGHT], t, 21, left)
            g8 = send(src, prm.at[t + 1, OPP], t, 22, opposite)
            a_phase(t + 1, 1, (OWN,))
            a_phase(t + 1, 0, (OWN,))
            g0.wait_recv()
            g2 = send(nxt.at[LEFT, a_rows], nxt.at[OPP, a_rows], t, 16, right)
            g3.wait_recv()
            g5 = send(nxt.at[RIGHT, b_rows], nxt.at[OPP, b_rows], t, 19, left)
            gather = [g0, g1, g2, g3, g4, g5, g6, g7, g8]
        else:
            def rows(shift, upper):
                q = lax.rem(chip + shift, n_chips)
                at = pl.multiple_of(core * half + q * kq + (kh if upper else 0), kh)
                return mean_out.at[pl.ds(at, kh)]

            def forward(shift, upper, idx, dev):
                return send(rows(shift, upper), rows(shift, upper), t, idx, dev)

            rows(0, False)[...] = mean_lo
            f0 = forward(0, False, 14, right)
            scat[2].wait_recv()
            scat[5].wait_recv()
            rows(0, True)[...] = (s_buf[t, 2 * OWN + 1] + rs_in[t, 2] + rs_in[t, 5]) / n_col[kh:]
            f3 = forward(0, True, 17, left)
            f1 = forward(0, True, 15, right)
            f4 = forward(0, False, 18, left)
            row_out[OWN, 0:1, :] = logw
            src = row_out.at[OWN]
            r6 = send(src, row_out.at[LEFT], t, 20, right)
            r7 = send(src, row_out.at[RIGHT], t, 21, left)
            r8 = send(src, row_out.at[OPP], t, 22, opposite)
            d2d = [forward(0, False, 23, partner), forward(0, True, 24, partner)]
            f0.wait_recv()
            f2 = forward(3, False, 16, right)
            d2d.append(forward(3, False, 25, partner))
            f3.wait_recv()
            f5 = forward(1, True, 19, left)
            d2d.append(forward(1, True, 26, partner))
            for c in (r6, r7, r8):
                c.wait_recv()
            rows_copy = send(row_out, row_in, t, 30, partner)
            f1.wait_recv()
            d2d.append(forward(3, True, 27, partner))
            f4.wait_recv()
            d2d.append(forward(1, False, 28, partner))
            f2.wait_recv()
            d2d.append(forward(2, False, 29, partner))
            f5.wait_recv()
            d2d.append(forward(2, True, 32, partner))
            rows_copy.wait_recv()
            for b in range(4):
                q = lax.rem(chip + SHIFT[b], n_chips)
                logw_out[pl.ds(core * n_chips + q, 1), :] = row_out[b, 0:1, :]
                logw_out[pl.ds((1 - core) * n_chips + q, 1), :] = row_in[b, 0:1, :]
            for c in d2d:
                c.wait_recv()
        drain()


def solution(mesh):
    n_pts, n_comp = mesh.shape["pts"], mesh.shape["comp"]
    n_chips = n_pts // CORES

    def per_device(points, means, log_w, inv_temp):
        n_loc, depth = points.shape
        k_loc = means.shape[0]
        kq = k_loc // n_pts
        half = n_chips * kq
        sweeps = inv_temp.shape[0]
        if n_chips != 4 or kq != LANES:
            raise ValueError("unsupported shape")
        f32, bf16 = jnp.float32, jnp.bfloat16
        kernel = functools.partial(
            em_kernel, sweeps, n_loc * n_pts, k_loc * n_comp, n_chips, n_comp
        )
        vmem = pl.BlockSpec(memory_space=pltpu.VMEM)
        anywhere = pl.BlockSpec(memory_space=pl.ANY)
        V = pltpu.VMEM
        mean, logw, lse = pl.pallas_call(
            kernel,
            out_shape=(
                jax.ShapeDtypeStruct((k_loc, depth), f32),
                jax.ShapeDtypeStruct((n_pts, kq), f32),
                jax.ShapeDtypeStruct((1, n_loc), f32),
            ),
            in_specs=[pl.BlockSpec(memory_space=pltpu.SMEM), anywhere, anywhere, vmem],
            out_specs=(vmem, vmem, vmem),
            scratch_shapes=[
                V((2, n_loc, depth), bf16),
                V((depth, 2 * n_loc), bf16),
                V((1, 2 * n_loc), f32),
                V((half, 2 * n_loc), f32),
                V((half, 2 * n_loc), bf16),
                V((4, kq, depth), f32),
                V((sweeps, 4, kq, depth), bf16),
                V((sweeps, 4, 8, kq), f32),
                V((4, 2 * n_loc), f32),
                V((4, 2 * n_loc), f32),
                V((sweeps, 2, n_loc), f32),
                V((sweeps, 2, n_loc), f32),
                V((sweeps, 2, n_loc), f32),
                V((sweeps, n_comp - 1, 2, n_loc), f32),
                V((sweeps, 1, n_loc), f32),
                V((sweeps, 1, n_loc), f32),
                V((sweeps, 8, kq // 2, depth), f32),
                V((sweeps, 6, kq // 2, depth), f32),
                V((sweeps, 2, kq // 2, depth), f32),
                V((sweeps, 4, 8, kq), f32),
                V((sweeps, 3, 8, kq), f32),
                V((4, 8, kq), f32),
                V((4, 8, kq), f32),
                pltpu.SemaphoreType.DMA((sweeps, 33)),
                pltpu.SemaphoreType.DMA((sweeps, 33)),
                pltpu.SemaphoreType.DMA((5,)),
            ],
            compiler_params=pltpu.CompilerParams(
                collective_id=0, has_side_effects=True, vmem_limit_bytes=60 * 1024 * 1024
            ),
            name="em",
        )(inv_temp, points, means, log_w.reshape(n_pts, kq))
        return mean, logw.reshape(k_loc), lse.reshape(n_loc)

    comp_spec = P(("fit", "comp"))
    return jax.shard_map(
        per_device,
        mesh=mesh,
        in_specs=(P(("fit", "pts"), None), P(("fit", "comp"), None), comp_spec, P()),
        out_specs=(P(("fit", "comp"), None), comp_spec, P(("fit", "pts"))),
        check_vma=False,
    )
```

```python
import contextlib
import functools
import math

import jax
import jax.numpy as jnp
from jax import lax
from jax.experimental import pallas as pl
from jax.experimental.pallas import tpu as pltpu
from jax.sharding import PartitionSpec as P

PRIOR_ALPHA = 1e-3
COUNT_EPS = 1e-6
LOG2E = math.log2(math.e)
LN2 = math.log(2.0)
MESH = pl.DeviceIdType.MESH
scope = contextlib.nullcontext
CORES = 2
LANES = 128

OPP, RIGHT, LEFT, OWN = range(4)
SHIFT = {OPP: 2, RIGHT: 1, LEFT: 3, OWN: 0}


def em_kernel(
    sweeps, n_total, k_total, n_chips, n_comp,
    beta_hbm, x_hbm, mean_hbm, logw_hbm,
    mean_out, logw_out, lse_out,
    beta_ref, logw_ref, x_all, xt, hq, e_buf, r_buf, mean_f, mean_b, prm, m_st, s_st, pair_out, pair_in, glob_out, glob_in,
    lse_own, lse_oth, cols_lp, cols_hm, raw_0, raw_1, s_buf, rs_in, acc_out, n_out, n_in, row_out, row_in, send_sem, recv_sem, copy_sem,
):
    raw = (raw_0, raw_1)
    n_loc, depth = x_all.shape[1], x_all.shape[2]
    kq = mean_f.shape[1]
    kh = kq // 2
    half = n_chips * kq

    p = lax.axis_index("pts")
    y = lax.axis_index("comp")
    chip = lax.div(p, CORES)
    core = p - chip * CORES
    partner = {"pts": chip * CORES + 1 - core}

    def x_peer(d):
        return {"pts": lax.rem(chip + d, n_chips) * CORES + core}

    right, left, opposite = x_peer(1), x_peer(n_chips - 1), x_peer(2)
    y_peers = [{"comp": lax.rem(y + d, n_comp)} for d in range(1, n_comp)]

    barrier = pltpu.get_barrier_semaphore()
    everyone = [partner, right, left, opposite] + y_peers
    for dev in everyone:
        pl.semaphore_signal(barrier, inc=1, device_id=dev, device_id_type=MESH)

    load_small = [
        pltpu.make_async_copy(logw_hbm, logw_ref, copy_sem.at[5]), pltpu.make_async_copy(beta_hbm, beta_ref, copy_sem.at[6])
    ]
    for c in load_small:
        c.start()
    load_mean = []
    for b in range(4):
        q = lax.rem(chip + SHIFT[b], n_chips)
        c = pltpu.make_async_copy(
            mean_hbm.at[pl.ds(pl.multiple_of(core * half + q * kq, kq), kq)], mean_f.at[b], copy_sem.at[b]
        )
        c.start()
        load_mean.append(c)

    load_x = pltpu.make_async_copy(x_hbm, x_all.at[0], copy_sem.at[4])
    load_x.start()

    pending = []

    def send(src, dst, t, idx, dev):
        c = pltpu.make_async_remote_copy(
            src_ref=src, dst_ref=dst, send_sem=send_sem.at[t, idx], recv_sem=recv_sem.at[t, idx],
            device_id=dev, device_id_type=MESH,
        )
        c.start()
        pending.append(c)
        return c

    def drain():
        for c in pending:
            c.wait_send()
        pending.clear()

    eye = lax.broadcasted_iota(jnp.int32, (kq, kq), 0) == lax.broadcasted_iota(jnp.int32, (kq, kq), 1)

    def to_col(row):
        return jnp.sum(jnp.where(eye, jnp.broadcast_to(row, (kq, kq)), 0.0), axis=1, keepdims=True)

    def to_row(col):
        return jnp.sum(jnp.where(eye, jnp.broadcast_to(col, (kq, kq)), 0.0), axis=0, keepdims=True)

    with scope("loads"):
        for c in load_small:
            c.wait()
    with scope("meanprep"):
        for b in range(4):
            load_mean[b].wait()
            mf = mean_f[b]
            mean_b[0, b] = mf.astype(jnp.bfloat16)
            q = lax.rem(chip + SHIFT[b], n_chips)
            prm[0, b, 0:1, :] = logw_ref[pl.ds(core * n_chips + q, 1), :] * LOG2E
            prm[0, b, 1:2, :] = to_row(0.5 * jnp.sum(mf * mf, axis=1, keepdims=True))

    tr = min(512, n_loc)
    n_tr = n_loc // tr

    def prepare(h, c):
        cols = slice(h * n_loc + c * tr, h * n_loc + (c + 1) * tr)
        blk = x_all[h, c * tr:(c + 1) * tr, :].T
        xt[:, cols] = blk
        f = blk.astype(jnp.float32)
        hq[:, cols] = 0.5 * jnp.sum(f * f, axis=0, keepdims=True)

    tile = min(256, n_loc)

    def columns(t, blocks):
        for b in blocks:
            cols_lp[b] = jnp.broadcast_to(to_col(prm[t, b, 0:1, :]), (kq, LANES))
            cols_hm[b] = jnp.broadcast_to(to_col(prm[t, b, 1:2, :]), (kq, LANES))

    def a_phase(t, tiles, blocks):
        neg_beta2 = beta_ref[t] * (-2.0 * LOG2E)
        lo, nb = blocks[0], len(blocks)
        means = mean_b.at[t, lo:lo + nb]

        def product(u):
            cols = slice(tiles[u] * tile, (tiles[u] + 1) * tile)
            raw[u % 2][0:nb * kq] = jnp.dot(
                means[...].reshape(nb * kq, depth), xt[:, cols], preferred_element_type=jnp.float32
            )

        product(0)
        for u in range(len(tiles)):
            if u + 1 < len(tiles):
                product(u + 1)
            for v in range(tile // LANES):
                at = tiles[u] * tile + v * LANES
                cols = slice(at, at + LANES)
                hqc = hq[:, cols]
                for i, b in enumerate(blocks):
                    a = raw[u % 2][i * kq:(i + 1) * kq, v * LANES:(v + 1) * LANES]
                    logit = ((hqc - a) + cols_hm[b]) * neg_beta2 + cols_lp[b]
                    m = jnp.max(logit, axis=0, keepdims=True)
                    e = jnp.exp2(logit - m)
                    e_buf[b * kq:(b + 1) * kq, cols] = e
                    m_st[b:b + 1, cols] = m
                    s_st[b:b + 1, cols] = jnp.sum(e, axis=0, keepdims=True)

    per_half = n_loc // tile
    tiles_of = [list(range(per_half)), list(range(per_half, 2 * per_half))]

    def local_pair(h):
        cols = pl.ds(h * n_loc, n_loc)
        ms = [m_st[b:b + 1, cols] for b in range(4)]
        m = jnp.maximum(jnp.maximum(ms[0], ms[1]), jnp.maximum(ms[2], ms[3]))
        s = sum(s_st[b:b + 1, cols] * jnp.exp2(ms[b] - m) for b in range(4))
        return m, s

    def r_phase(h, blocks, lse, accs):
        rt = min(512, n_loc)

        def body(c, acc):
            acc = list(acc)
            cols = pl.ds(pl.multiple_of(h * n_loc + c * rt, rt), rt)
            l2 = lse[:, pl.ds(pl.multiple_of(c * rt, rt), rt)]
            for i, b in enumerate(blocks):
                f = jnp.exp2(m_st[b:b + 1, cols] - l2)
                r = e_buf[b * kq:(b + 1) * kq, cols] * f
                r_buf[b * kq:(b + 1) * kq, cols] = r.astype(jnp.bfloat16)
                for v in range(rt // LANES):
                    acc[i] = acc[i] + r[:, v * LANES:(v + 1) * LANES]
            return tuple(acc)

        return lax.fori_loop(0, n_loc // rt, body, accs)

    zero = jnp.zeros((kq, LANES), jnp.float32)

    for t in range(sweeps):
        last = t == sweeps - 1
        if t == 0:
            columns(0, range(4))
            with scope("loadx"):
                load_x.wait()
            with scope("prep0"):
                for c in range(n_tr):
                    prepare(0, c)
            with scope("barrier"):
                pl.semaphore_wait(barrier, len(everyone))
            x_rows = [pl.ds(c * tr, tr) for c in range(n_tr)]
            x_copies = [send(x_hbm.at[r], x_all.at[1, r], 0, 33 + c, partner) for c, r in enumerate(x_rows)]
            with scope("a00"):
                a_phase(t, tiles_of[0], range(4))
            per_tr = tr // tile
            for c in range(n_tr):
                with scope("xwait"):
                    x_copies[c].wait_recv()
                with scope("prep1"):
                    prepare(1, c)
                with scope("a01"):
                    a_phase(t, tiles_of[1][c * per_tr:(c + 1) * per_tr], range(4))
        else:
            with scope("wait_left"):
                gather[1].wait_recv()
                gather[6].wait_recv()
            with scope("wait_right"):
                gather[4].wait_recv()
                gather[7].wait_recv()
            with scope("a_right"):
                columns(t, (RIGHT, LEFT))
                a_phase(t, tiles_of[1] + tiles_of[0], (RIGHT, LEFT))
            with scope("wait_opp"):
                gather[2].wait_recv()
                gather[5].wait_recv()
                gather[8].wait_recv()
            with scope("a_opp1"):
                columns(t, (OPP,))
                a_phase(t, tiles_of[1], (OPP,))
        m, s = local_pair(1)
        pair_out[t, 0:1, :] = m
        pair_out[t, 1:2, :] = s
        pair = send(pair_out.at[t], pair_in.at[t], t, 0, partner)
        if t > 0:
            with scope("a_opp0"):
                a_phase(t, tiles_of[0], (OPP,))
        m, s = local_pair(0)
        with scope("wait_pair"):
            pair.wait_recv()
        m1, s1 = pair_in[t, 0:1, :], pair_in[t, 1:2, :]
        top = jnp.maximum(m, m1)
        s = s * jnp.exp2(m - top) + s1 * jnp.exp2(m1 - top)
        glob_out[t, 0:1, :] = top
        glob_out[t, 1:2, :] = s
        across = [
            send(glob_out.at[t], glob_in.at[t, d], t, 1 + d, y_peers[d]) for d in range(n_comp - 1)
        ]
        tops, sums = [top], [s]
        for d in range(n_comp - 1):
            with scope("wait_y"):
                across[d].wait_recv()
            tops.append(glob_in[t, d, 0:1, :])
            sums.append(glob_in[t, d, 1:2, :])
        top = functools.reduce(jnp.maximum, tops)
        total = sum(v * jnp.exp2(w - top) for v, w in zip(sums, tops))
        lse2 = top + jnp.log(total) * LOG2E
        lse_own[t] = lse2
        swap = send(lse_own.at[t], lse_oth.at[t], t, 4, partner)
        if last:
            lse = lse2 * LN2
            for i in range(n_loc // LANES):
                lse_out[i:i + 1, :] = lse[:, i * LANES:(i + 1) * LANES]

        own_r = lse_own.at[t]
        with scope("r_own"):
            accs = r_phase(0, (0, 1, 2, 3), own_r, (zero,) * 4)
        with scope("wait_swap"):
            swap.wait_recv()
        oth_r = lse_oth.at[t]
        with scope("r_oth_a"):
            acc_a = r_phase(1, (0, 1), oth_r, accs[:2])
        counts = []

        def stats(lo):
            out = jnp.dot(
                r_buf[lo * kq:(lo + 2) * kq, 0:n_loc], x_all[0], preferred_element_type=jnp.float32
            )
            out += jnp.dot(
                r_buf[lo * kq:(lo + 2) * kq, n_loc:2 * n_loc], x_all[1], preferred_element_type=jnp.float32
            )
            s_buf[t, 2 * lo:2 * lo + 4] = out.reshape(4, kh, depth)

        with scope("stats0"):
            stats(0)
        scat = [
            send(s_buf.at[t, 2 * OPP], rs_in.at[t, 0], t, 5, right),
            send(s_buf.at[t, 2 * OPP + 1], rs_in.at[t, 1], t, 6, left),
        ]
        with scope("r_oth_b"):
            acc_b = r_phase(1, (2, 3), oth_r, accs[2:])
        for b, acc in enumerate(tuple(acc_a) + tuple(acc_b)):
            row = to_row(jnp.sum(acc, axis=1, keepdims=True))
            n_out[t, b, 0:1, :] = row
            counts.append(row)
        n_copies = [
            send(n_out.at[t, OPP], n_in.at[t, 0], t, 8, opposite),
            send(n_out.at[t, RIGHT], n_in.at[t, 1], t, 9, right),
            send(n_out.at[t, LEFT], n_in.at[t, 2], t, 10, left),
        ]
        with scope("stats2"):
            stats(2)
        with scope("wait_out"):
            for c in scat:
                c.wait_send()
                pending[:] = [d for d in pending if d is not c]
        scat.append(send(s_buf.at[t, 2 * RIGHT + 1], rs_in.at[t, 2], t, 7, right))
        scat.append(send(s_buf.at[t, 2 * LEFT], rs_in.at[t, 3], t, 11, left))
        with scope("wait_s0"):
            scat[0].wait_recv()
        acc_out[t, 0] = s_buf[t, 2 * RIGHT] + rs_in[t, 0]
        scat.append(send(acc_out.at[t, 0], rs_in.at[t, 4], t, 12, right))
        with scope("wait_s1"):
            scat[1].wait_recv()
        acc_out[t, 1] = s_buf[t, 2 * LEFT + 1] + rs_in[t, 1]
        scat.append(send(acc_out.at[t, 1], rs_in.at[t, 5], t, 13, left))

        n_row = counts[OWN]
        for d in range(3):
            n_copies[d].wait_recv()
            n_row = n_row + n_in[t, d, 0:1, :]
        n_col = to_col(n_row) + COUNT_EPS
        logw = jnp.log((n_row + PRIOR_ALPHA) / (n_total + k_total * PRIOR_ALPHA))

        with scope("wait_s34"):
            scat[3].wait_recv()
            scat[4].wait_recv()
        mean_lo = (s_buf[t, 2 * OWN] + rs_in[t, 3] + rs_in[t, 4]) / n_col[:kh]
        if not last:
            nxt = mean_b.at[t + 1]
            a_rows, b_rows = pl.ds(0, kh), pl.ds(kh, kh)
            mean_b[t + 1, OWN, 0:kh, :] = mean_lo.astype(jnp.bfloat16)
            mine_a, mine_b = nxt.at[OWN, a_rows], nxt.at[OWN, b_rows]
            g0 = send(mine_a, nxt.at[LEFT, a_rows], t, 14, right)
            with scope("wait_s25"):
                scat[2].wait_recv()
                scat[5].wait_recv()
            mean_hi = (s_buf[t, 2 * OWN + 1] + rs_in[t, 2] + rs_in[t, 5]) / n_col[kh:]
            mean_b[t + 1, OWN, kh:kq, :] = mean_hi.astype(jnp.bfloat16)
            g3 = send(mine_b, nxt.at[RIGHT, b_rows], t, 17, left)
            g1 = send(mine_b, nxt.at[LEFT, b_rows], t, 15, right)
            g4 = send(mine_a, nxt.at[RIGHT, a_rows], t, 18, left)
            sq = jnp.concatenate(
                [jnp.sum(mean_lo * mean_lo, axis=1, keepdims=True), jnp.sum(mean_hi * mean_hi, axis=1, keepdims=True)], axis=0
            )
            prm[t + 1, OWN, 0:1, :] = logw * LOG2E
            prm[t + 1, OWN, 1:2, :] = to_row(0.5 * sq)
            src = prm.at[t + 1, OWN]
            g6 = send(src, prm.at[t + 1, LEFT], t, 20, right)
            g7 = send(src, prm.at[t + 1, RIGHT], t, 21, left)
            g8 = send(src, prm.at[t + 1, OPP], t, 22, opposite)
            with scope("a_own"):
                columns(t + 1, (OWN,))
                a_phase(t + 1, tiles_of[1] + tiles_of[0], (OWN,))
            with scope("wait_g0"):
                g0.wait_recv()
            g2 = send(nxt.at[LEFT, a_rows], nxt.at[OPP, a_rows], t, 16, right)
            with scope("wait_g3"):
                g3.wait_recv()
            g5 = send(nxt.at[RIGHT, b_rows], nxt.at[OPP, b_rows], t, 19, left)
            gather = [g0, g1, g2, g3, g4, g5, g6, g7, g8]
        else:
            def rows(shift, upper):
                q = lax.rem(chip + shift, n_chips)
                at = pl.multiple_of(core * half + q * kq + (kh if upper else 0), kh)
                return mean_out.at[pl.ds(at, kh)]

            def forward(shift, upper, idx, dev):
                return send(rows(shift, upper), rows(shift, upper), t, idx, dev)

            rows(0, False)[...] = mean_lo
            f0 = forward(0, False, 14, right)
            with scope("wait_s25"):
                scat[2].wait_recv()
                scat[5].wait_recv()
            rows(0, True)[...] = (s_buf[t, 2 * OWN + 1] + rs_in[t, 2] + rs_in[t, 5]) / n_col[kh:]
            f3 = forward(0, True, 17, left)
            f1 = forward(0, True, 15, right)
            f4 = forward(0, False, 18, left)
            row_out[OWN, 0:1, :] = logw
            src = row_out.at[OWN]
            r6 = send(src, row_out.at[LEFT], t, 20, right)
            r7 = send(src, row_out.at[RIGHT], t, 21, left)
            r8 = send(src, row_out.at[OPP], t, 22, opposite)
            d2d = [forward(0, False, 23, partner), forward(0, True, 24, partner)]
            with scope("wait_f0"):
                f0.wait_recv()
            f2 = forward(3, False, 16, right)
            d2d.append(forward(3, False, 25, partner))
            with scope("wait_f3"):
                f3.wait_recv()
            f5 = forward(1, True, 19, left)
            d2d.append(forward(1, True, 26, partner))
            for c in (r6, r7, r8):
                c.wait_recv()
            rows_copy = send(row_out, row_in, t, 30, partner)
            with scope("wait_f1"):
                f1.wait_recv()
            d2d.append(forward(3, True, 27, partner))
            with scope("wait_f4"):
                f4.wait_recv()
            d2d.append(forward(1, False, 28, partner))
            with scope("wait_f2"):
                f2.wait_recv()
            d2d.append(forward(2, False, 29, partner))
            with scope("wait_f5"):
                f5.wait_recv()
            d2d.append(forward(2, True, 32, partner))
            with scope("wait_rows"):
                rows_copy.wait_recv()
            for b in range(4):
                q = lax.rem(chip + SHIFT[b], n_chips)
                logw_out[pl.ds(core * n_chips + q, 1), :] = row_out[b, 0:1, :]
                logw_out[pl.ds((1 - core) * n_chips + q, 1), :] = row_in[b, 0:1, :]
            with scope("wait_d2d"):
                for c in d2d:
                    c.wait_recv()
    with scope("drain"):
        drain()


def solution(mesh):
    n_pts, n_comp = mesh.shape["pts"], mesh.shape["comp"]
    n_chips = n_pts // CORES

    def per_device(points, means, log_w, inv_temp):
        n_loc, depth = points.shape
        k_loc = means.shape[0]
        kq = k_loc // n_pts
        half = n_chips * kq
        sweeps = inv_temp.shape[0]
        if n_chips != 4 or kq != LANES:
            raise ValueError("unsupported shape")
        f32, bf16 = jnp.float32, jnp.bfloat16
        kernel = functools.partial(
            em_kernel, sweeps, n_loc * n_pts, k_loc * n_comp, n_chips, n_comp
        )
        vmem = pl.BlockSpec(memory_space=pltpu.VMEM)
        hbm = pl.BlockSpec(memory_space=pltpu.HBM)
        V = pltpu.VMEM
        mean, logw, lse = pl.pallas_call(
            kernel,
            out_shape=(
                jax.ShapeDtypeStruct((k_loc, depth), f32),
                jax.ShapeDtypeStruct((n_pts, kq), f32),
                jax.ShapeDtypeStruct((n_loc // LANES, LANES), f32),
            ),
            in_specs=[hbm] * 4,
            out_specs=(vmem, vmem, vmem),
            scratch_shapes=[
                pltpu.SMEM((sweeps,), f32),
                V((n_pts, kq), f32),
                V((2, n_loc, depth), bf16),
                V((depth, 2 * n_loc), bf16),
                V((1, 2 * n_loc), f32),
                V((half, 2 * n_loc), f32),
                V((half, 2 * n_loc), bf16),
                V((4, kq, depth), f32),
                V((sweeps, 4, kq, depth), bf16),
                V((sweeps, 4, 8, kq), f32),
                V((4, 2 * n_loc), f32),
                V((4, 2 * n_loc), f32),
                V((sweeps, 2, n_loc), f32),
                V((sweeps, 2, n_loc), f32),
                V((sweeps, 2, n_loc), f32),
                V((sweeps, n_comp - 1, 2, n_loc), f32),
                V((sweeps, 1, n_loc), f32),
                V((sweeps, 1, n_loc), f32),
                V((4, kq, LANES), f32),
                V((4, kq, LANES), f32),
                V((half, min(256, n_loc)), f32),
                V((half, min(256, n_loc)), f32),
                V((sweeps, 8, kq // 2, depth), f32),
                V((sweeps, 6, kq // 2, depth), f32),
                V((sweeps, 2, kq // 2, depth), f32),
                V((sweeps, 4, 8, kq), f32),
                V((sweeps, 3, 8, kq), f32),
                V((4, 8, kq), f32),
                V((4, 8, kq), f32),
                pltpu.SemaphoreType.DMA((sweeps, 40)),
                pltpu.SemaphoreType.DMA((sweeps, 40)),
                pltpu.SemaphoreType.DMA((7,)),
            ],
            compiler_params=pltpu.CompilerParams(
                collective_id=0, has_side_effects=True, vmem_limit_bytes=44 * 1024 * 1024
            ),
            name="em",
        )(*(pltpu.with_memory_space_constraint(v, pltpu.HBM) for v in (inv_temp, points, means, log_w.reshape(n_pts, kq))))
        return mean, logw.reshape(k_loc), lse.reshape(n_loc)

    comp_spec = P(("fit", "comp"))
    return jax.shard_map(
        per_device,
        mesh=mesh,
        in_specs=(P(("fit", "pts"), None), P(("fit", "comp"), None), comp_spec, P()),
        out_specs=(P(("fit", "comp"), None), comp_spec, P(("fit", "pts"))),
        check_vma=False,
    )
```

```python
import contextlib
import functools
import math

import jax
import jax.numpy as jnp
from jax import lax
from jax.experimental import pallas as pl
from jax.experimental.pallas import tpu as pltpu
from jax.sharding import PartitionSpec as P

PRIOR_ALPHA = 1e-3
COUNT_EPS = 1e-6
LOG2E = math.log2(math.e)
LN2 = math.log(2.0)
MESH = pl.DeviceIdType.MESH
scope = contextlib.nullcontext
CORES = 2
PARTS = 4
DIRECT = 0
LANES = 128

OPP, RIGHT, LEFT, OWN = range(4)
SHIFT = {OPP: 2, RIGHT: 1, LEFT: 3, OWN: 0}

PAIR, SWAP, COUNT, ROW, FINAL, XPART, PIECES = 0, 1, 2, 5, 9, 10, 14
FAR_A, FAR_B, NEAR_A, NEAR_B, SUM_A, SUM_B, OWN_A_RIGHT, OWN_B_RIGHT, OWN_A_LEFT, OWN_B_LEFT, ON_A, ON_B = range(
    PIECES, PIECES + 12 * PARTS, PARTS
)
ACROSS = PIECES + 12 * PARTS
SUMS_RIGHT, SUMS_LEFT, MEANS_RIGHT, MEANS_LEFT, X_OUT, FINAL_OUT, SINGLE = range(7)


def em_kernel(
    sweeps, n_total, k_total, n_chips, n_comp,
    beta_hbm, x_hbm, mean_hbm, logw_hbm,
    mean_out, logw_out, lse_out,
    beta_ref, logw_ref, x_all, xt, x_sq, e_buf, r_buf, mean_f, mean_b, prm, m_st, s_st, factor, pair_out, pair_in, glob_out, glob_in,
    lse_own, lse_oth, cols_c, raw_0, raw_1, n_acc, s_buf, rs_in, acc_out, n_out, n_in, row_out, row_in, send_sem, recv_sem, copy_sem,
):
    raw = (raw_0, raw_1)
    n_loc, depth = x_all.shape[1], x_all.shape[2]
    kq = mean_f.shape[1]
    kh, kp = kq // 2, kq // 2 // PARTS
    half = n_chips * kq

    p = lax.axis_index("pts")
    y = lax.axis_index("comp")
    chip = lax.div(p, CORES)
    core = p - chip * CORES
    partner = {"pts": chip * CORES + 1 - core}

    def x_peer(d):
        return {"pts": lax.rem(chip + d, n_chips) * CORES + core}

    right, left, opposite = x_peer(1), x_peer(n_chips - 1), x_peer(2)
    y_order = sorted(range(1, n_comp), key=lambda d: -min(d, n_comp - d))
    y_peers = [{"comp": lax.rem(y + d, n_comp)} for d in y_order]

    barrier = pltpu.get_barrier_semaphore()
    everyone = [partner, right, left, opposite] + y_peers
    for dev in everyone:
        pl.semaphore_signal(barrier, inc=1, device_id=dev, device_id_type=MESH)

    load_small = [
        pltpu.make_async_copy(logw_hbm, logw_ref, copy_sem.at[5]), pltpu.make_async_copy(beta_hbm, beta_ref, copy_sem.at[6])
    ]
    for c in load_small:
        c.start()
    load_mean = []
    for b in range(4):
        q = lax.rem(chip + SHIFT[b], n_chips)
        c = pltpu.make_async_copy(
            mean_hbm.at[pl.ds(pl.multiple_of(core * half + q * kq, kq), kq)], mean_f.at[b], copy_sem.at[b]
        )
        c.start()
        load_mean.append(c)

    load_x = pltpu.make_async_copy(x_hbm, x_all.at[0], copy_sem.at[4])
    load_x.start()

    pending = {}

    def send(src, dst, arrive, depart, dev, when=None):
        c = pltpu.make_async_remote_copy(
            src_ref=src, dst_ref=dst, send_sem=send_sem.at[depart], recv_sem=recv_sem.at[arrive],
            device_id=dev, device_id_type=MESH,
        )
        if depart >= SINGLE:
            if depart in pending:
                pending[depart].wait_send()
            pending[depart] = c
        if when is None:
            c.start()
        else:
            pl.when(when)(c.start)
        return c

    def wait_group(depart, ref):
        pltpu.make_async_remote_copy(
            src_ref=ref, dst_ref=ref, send_sem=send_sem.at[depart], recv_sem=recv_sem.at[PAIR],
            device_id=partner, device_id_type=MESH,
        ).wait_send()

    def wait_sums(t):
        wait_group(SUMS_RIGHT, rs_in.at[t, pl.ds(0, 3)])
        wait_group(SUMS_LEFT, rs_in.at[t, pl.ds(0, 3)])

    def wait_means(t):
        ref = mean_b.at[t + 1, pl.ds(0, 3), pl.ds(0, kh)] if t < sweeps - 1 else mean_out.at[pl.ds(0, 3 * kh)]
        wait_group(MEANS_RIGHT, ref)
        wait_group(MEANS_LEFT, ref)

    eye = lax.broadcasted_iota(jnp.int32, (kq, kq), 0) == lax.broadcasted_iota(jnp.int32, (kq, kq), 1)

    def to_col(row):
        return jnp.sum(jnp.where(eye, jnp.broadcast_to(row, (kq, kq)), 0.0), axis=1, keepdims=True)

    def to_row(col):
        return jnp.sum(jnp.where(eye, jnp.broadcast_to(col, (kq, kq)), 0.0), axis=0, keepdims=True)

    with scope("loads"):
        for c in load_small:
            c.wait()
    tr = min(512, n_loc)
    n_tr = n_loc // tr
    with scope("barrier"):
        pl.semaphore_wait(barrier, len(everyone))
    x_rows = [pl.ds(c * tr, tr) for c in range(n_tr)]
    x_copies = [send(x_hbm.at[r], x_all.at[1, r], XPART + c, X_OUT, partner) for c, r in enumerate(x_rows)]
    with scope("meanprep"):
        for b in range(4):
            load_mean[b].wait()
            mf = mean_f[b]
            mean_b[0, b] = mf.astype(jnp.bfloat16)
            q = lax.rem(chip + SHIFT[b], n_chips)
            prm[0, b, 0:1, :] = logw_ref[pl.ds(core * n_chips + q, 1), :]
            prm[0, b, 1:2, :] = to_row(jnp.sum(mf * mf, axis=1, keepdims=True))

    def prepare(h, c):
        cols = slice(h * n_loc + c * tr, h * n_loc + (c + 1) * tr)
        blk = x_all[h, c * tr:(c + 1) * tr, :].T
        xt[:, cols] = blk
        if h == 0:
            f = blk.astype(jnp.float32)
            x_sq[:, cols] = jnp.sum(f * f, axis=0, keepdims=True)

    tile = min(256, n_loc)

    def columns(t, blocks):
        for b in blocks:
            row = (prm[t, b, 0:1, :] - beta_ref[t] * prm[t, b, 1:2, :]) * LOG2E
            cols_c[b] = jnp.broadcast_to(to_col(row), (kq, LANES))

    def a_phase(t, tiles, blocks):
        slope = beta_ref[t] * (2.0 * LOG2E)
        lo, nb = blocks[0], len(blocks)
        means = mean_b.at[t, lo:lo + nb]

        def product(u):
            cols = slice(tiles[u] * tile, (tiles[u] + 1) * tile)
            raw[u % 2][0:nb * kq] = jnp.dot(
                means[...].reshape(nb * kq, depth), xt[:, cols], preferred_element_type=jnp.float32
            )

        product(0)
        for u in range(len(tiles)):
            if u + 1 < len(tiles):
                product(u + 1)
            for v in range(tile // LANES):
                at = tiles[u] * tile + v * LANES
                cols = slice(at, at + LANES)
                for i, b in enumerate(blocks):
                    a = raw[u % 2][i * kq:(i + 1) * kq, v * LANES:(v + 1) * LANES]
                    logit = a * slope + cols_c[b]
                    m = jnp.max(logit, axis=0, keepdims=True)
                    e = jnp.exp2(logit - m)
                    e_buf[b * kq:(b + 1) * kq, cols] = e
                    m_st[b:b + 1, cols] = m
                    s_st[b:b + 1, cols] = jnp.sum(e, axis=0, keepdims=True)

    per_half = n_loc // tile
    tiles_of = [list(range(per_half)), list(range(per_half, 2 * per_half))]

    def local_pair(h):
        cols = pl.ds(h * n_loc, n_loc)
        ms = [m_st[b:b + 1, cols] for b in range(4)]
        m = jnp.maximum(jnp.maximum(ms[0], ms[1]), jnp.maximum(ms[2], ms[3]))
        s = sum(s_st[b:b + 1, cols] * jnp.exp2(ms[b] - m) for b in range(4))
        return m, s

    def r_phase(h, blocks, lse):
        half_cols = slice(h * n_loc, (h + 1) * n_loc)
        if 0 in blocks:
            factor[:, half_cols] = jnp.exp2(m_st[:, half_cols] - lse[...])
        accs = [jnp.zeros((kq, LANES), jnp.float32) for _ in blocks]
        for c in range(n_loc // LANES):
            cols = slice(h * n_loc + c * LANES, h * n_loc + (c + 1) * LANES)
            for i, b in enumerate(blocks):
                r = e_buf[b * kq:(b + 1) * kq, cols] * factor[b:b + 1, cols]
                r_buf[b * kq:(b + 1) * kq, cols] = r.astype(jnp.bfloat16)
                accs[i] = accs[i] + r
        for i, b in enumerate(blocks):
            n_acc[h, b] = accs[i]

    def stats(h, lo):
        out = jnp.dot(
            r_buf[lo * kq:(lo + 2) * kq, h * n_loc:(h + 1) * n_loc], x_all[h], preferred_element_type=jnp.float32
        ).reshape(4, kh, depth)
        if h == 0:
            s_buf[t, 2 * lo:2 * lo + 4] = out
        else:
            s_buf[t, 2 * lo:2 * lo + 4] += out

    for t in range(sweeps):
        last = t == sweeps - 1
        if t == 0:
            columns(0, range(4))
            with scope("loadx"):
                load_x.wait()
            with scope("prep0"):
                for c in range(n_tr):
                    prepare(0, c)
            with scope("a00"):
                a_phase(t, tiles_of[0], range(4))
            per_tr = tr // tile
            for c in range(n_tr):
                with scope("xwait"):
                    x_copies[c].wait_recv()
                with scope("prep1"):
                    prepare(1, c)
                with scope("a01"):
                    a_phase(t, tiles_of[1][c * per_tr:(c + 1) * per_tr], range(4))
        else:
            with scope("wait_near"):
                for c in b_right + a_left + rows[:2]:
                    c.wait_recv()
            with scope("a_right"):
                columns(t, (RIGHT, LEFT))
                a_phase(t, tiles_of[1] + tiles_of[0], (RIGHT, LEFT))
            with scope("wait_opp"):
                for c in a_on + b_on + rows[2:]:
                    c.wait_recv()
            with scope("a_opp1"):
                columns(t, (OPP,))
                a_phase(t, tiles_of[1], (OPP,))
        m, s = local_pair(1)
        pair_out[t, 0:1, :] = m
        pair_out[t, 1:2, :] = s
        pair = send(pair_out.at[t], pair_in.at[t], PAIR, SINGLE, partner)
        if t > 0:
            with scope("a_opp0"):
                a_phase(t, tiles_of[0], (OPP,))
        m, s = local_pair(0)
        with scope("wait_pair"):
            pair.wait_recv()
        m1, s1 = pair_in[t, 0:1, :], pair_in[t, 1:2, :]
        top = jnp.maximum(m, m1)
        s = s * jnp.exp2(m - top) + s1 * jnp.exp2(m1 - top)
        glob_out[t, 0:1, :] = top
        glob_out[t, 1:2, :] = s
        across = [
            send(glob_out.at[t], glob_in.at[t, d], ACROSS + t * (n_comp - 1) + d, SINGLE + 9 + d, y_peers[d])
            for d in range(n_comp - 1)
        ]
        tops, sums = [top], [s]
        for d in reversed(range(n_comp - 1)):
            with scope("wait_y"):
                across[d].wait_recv()
            tops.append(glob_in[t, d, 0:1, :])
            sums.append(glob_in[t, d, 1:2, :])
        top = functools.reduce(jnp.maximum, tops)
        total = sum(v * jnp.exp2(w - top) for v, w in zip(sums, tops))
        lse2 = top + jnp.log(total) * LOG2E
        lse_own[t] = lse2
        swap = send(lse_own.at[t], lse_oth.at[t], SWAP, SINGLE + 1, partner)
        if last:
            lse = lse2 * LN2 - beta_ref[t] * x_sq[...]
            for i in range(n_loc // LANES):
                lse_out[i:i + 1, :] = lse[:, i * LANES:(i + 1) * LANES]

        own_r, oth_r = lse_own.at[t], lse_oth.at[t]
        with scope("r_own_a"):
            r_phase(0, (0, 1), own_r)
        with scope("stats0"):
            stats(0, 0)
        with scope("wait_swap"):
            swap.wait_recv()
        with scope("r_oth_a"):
            r_phase(1, (0, 1), oth_r)
        with scope("stats1"):
            stats(1, 0)

        parts = [pl.ds(i * kp, kp) for i in range(PARTS)]

        def s_piece(b, half_b, i):
            return s_buf.at[t, 2 * b + half_b, parts[i]]

        def in_piece(slot, i):
            return rs_in.at[t, slot, parts[i]]

        def near_b_send(i, when=None):
            return send(s_piece(RIGHT, 1, i), in_piece(2, i), NEAR_B + i, SUMS_RIGHT, right, when)

        def near_a_send(i):
            return send(s_piece(LEFT, 0, i), in_piece(3, i), NEAR_A + i, SUMS_LEFT, left)

        def first_sends(when):
            a, b = [], []
            for i in range(PARTS):
                a.append(send(s_piece(OPP, 0, i), in_piece(0, i), FAR_A + i, SUMS_RIGHT, right, when))
                b.append(send(s_piece(OPP, 1, i), in_piece(1, i), FAR_B + i, SUMS_LEFT, left, when))
            return a, b, [near_b_send(i, when) for i in range(2)]

        if t > 0:
            wait_sums(t - 1)
        far_a, far_b, near_b = first_sends(core == 0)
        with scope("r_23"):
            r_phase(0, (2, 3), own_r)
            r_phase(1, (2, 3), oth_r)
        counts = []
        for b in range(4):
            row = to_row(jnp.sum(n_acc[0, b] + n_acc[1, b], axis=1, keepdims=True))
            n_out[t, b, 0:1, :] = row
            counts.append(row)
        n_copies = [
            send(n_out.at[t, b], n_in.at[t, d], COUNT + d, SINGLE + 2 + d, dev)
            for d, (b, dev) in enumerate(((OPP, opposite), (RIGHT, right), (LEFT, left)))
        ]
        with scope("stats2"):
            stats(0, 2)
            stats(1, 2)
        first_sends(core == 1)
        near_a = [near_a_send(i) for i in range(2)]
        sum_a, sum_b = [], []
        for i in range(PARTS):
            with scope("wait_far_a"):
                far_a[i].wait_recv()
            acc_out[t, 0, parts[i]] = s_buf[t, 2 * RIGHT, parts[i]] + rs_in[t, 0, parts[i]]
            sum_a.append(send(acc_out.at[t, 0, parts[i]], in_piece(4, i), SUM_A + i, SUMS_RIGHT, right))
            if i + 2 < PARTS:
                near_b.append(near_b_send(i + 2))
            with scope("wait_far_b"):
                far_b[i].wait_recv()
            acc_out[t, 1, parts[i]] = s_buf[t, 2 * LEFT + 1, parts[i]] + rs_in[t, 1, parts[i]]
            sum_b.append(send(acc_out.at[t, 1, parts[i]], in_piece(5, i), SUM_B + i, SUMS_LEFT, left))
            if i + 2 < PARTS:
                near_a.append(near_a_send(i + 2))

        n_row = counts[OWN]
        for d in range(3):
            with scope("wait_n"):
                n_copies[d].wait_recv()
            n_row = n_row + n_in[t, d, 0:1, :]
        n_col = to_col(n_row) + COUNT_EPS
        logw = jnp.log((n_row + PRIOR_ALPHA) / (n_total + k_total * PRIOR_ALPHA))

        def m_piece(b, half_b, i):
            at = half_b * kh + i * kp
            if not last:
                return mean_b.at[t + 1, b, pl.ds(at, kp)]
            q = lax.rem(chip + SHIFT[b], n_chips)
            return mean_out.at[pl.ds(pl.multiple_of(core * half + q * kq + at, kp), kp)]

        def m_send(b, there, half_b, i, arrive, dev):
            depart = MEANS_LEFT if arrive >= OWN_A_LEFT and not ON_A <= arrive < ON_B else MEANS_RIGHT
            return send(m_piece(b, half_b, i), m_piece(b if last else there, half_b, i), arrive, depart, dev)

        def swap_piece(b, half_b, i):
            if last:
                send(m_piece(b, half_b, i), m_piece(b, half_b, i), FINAL, FINAL_OUT, partner)

        if t > 0:
            wait_means(t - 1)
        sq = {}
        a_right, b_right, a_left, b_left, a_on, b_on, a_direct, b_direct = ([] for _ in range(8))
        for i in range(PARTS):
            for half_b, far, near, slots in ((0, sum_a, near_a, (3, 4)), (1, sum_b, near_b, (2, 5))):
                with scope("wait_sum"):
                    near[i].wait_recv()
                    far[i].wait_recv()
                at = half_b * kh + i * kp
                mean = (
                    s_buf[t, 2 * OWN + half_b, parts[i]] + rs_in[t, slots[0], parts[i]] + rs_in[t, slots[1], parts[i]]
                ) / n_col[at:at + kp]
                m_piece(OWN, half_b, i)[...] = mean if last else mean.astype(jnp.bfloat16)
                sq[half_b, i] = jnp.sum(mean * mean, axis=1, keepdims=True)
                if half_b == 0:
                    a_right.append(m_send(OWN, LEFT, 0, i, OWN_A_RIGHT + i, right))
                else:
                    b_left.append(m_send(OWN, RIGHT, 1, i, OWN_B_LEFT + i, left))
            b_right.append(m_send(OWN, LEFT, 1, i, OWN_B_RIGHT + i, right))
            a_left.append(m_send(OWN, RIGHT, 0, i, OWN_A_LEFT + i, left))
            if i >= PARTS - DIRECT:
                a_direct.append(m_send(OWN, OPP, 0, i, ON_A + i, opposite))
                b_direct.append(m_send(OWN, OPP, 1, i, ON_B + i, opposite))
            swap_piece(OWN, 0, i)
            swap_piece(OWN, 1, i)

        own_row, to_rows = (row_out.at[OWN], row_out) if last else (prm.at[t + 1, OWN], prm.at[t + 1])
        own_row[0:1, :] = logw
        if not last:
            col = jnp.concatenate([sq[h, i] for h in range(2) for i in range(PARTS)], axis=0)
            own_row[1:2, :] = to_row(col)
        rows = [
            send(own_row, to_rows.at[LEFT], ROW, SINGLE + 5, right),
            send(own_row, to_rows.at[RIGHT], ROW + 1, SINGLE + 6, left),
            send(own_row, to_rows.at[OPP], ROW + 2, SINGLE + 7, opposite),
        ]
        if not last:
            with scope("a_own"):
                columns(t + 1, (OWN,))
                a_phase(t + 1, tiles_of[1] + tiles_of[0], (OWN,))
        for i in range(PARTS):
            with scope("wait_on_a"):
                a_right[i].wait_recv()
            if i < PARTS - DIRECT:
                a_on.append(m_send(LEFT, OPP, 0, i, ON_A + i, right))
            with scope("wait_on_b"):
                b_left[i].wait_recv()
            if i < PARTS - DIRECT:
                b_on.append(m_send(RIGHT, OPP, 1, i, ON_B + i, left))
            swap_piece(LEFT, 0, i)
            swap_piece(RIGHT, 1, i)
        a_on += a_direct
        b_on += b_direct
        if last:
            with scope("wait_rows"):
                for c in rows:
                    c.wait_recv()
            rows_copy = send(row_out, row_in, ROW + 3, SINGLE + 8, partner)
            for i in range(PARTS):
                with scope("wait_bl"):
                    b_right[i].wait_recv()
                swap_piece(LEFT, 1, i)
                with scope("wait_ar"):
                    a_left[i].wait_recv()
                swap_piece(RIGHT, 0, i)
            for i in range(PARTS):
                with scope("wait_oa"):
                    a_on[i].wait_recv()
                swap_piece(OPP, 0, i)
                with scope("wait_ob"):
                    b_on[i].wait_recv()
                swap_piece(OPP, 1, i)
            with scope("wait_d2dr"):
                rows_copy.wait_recv()
            for b in range(4):
                q = lax.rem(chip + SHIFT[b], n_chips)
                logw_out[pl.ds(core * n_chips + q, 1), :] = row_out[b, 0:1, :]
                logw_out[pl.ds((1 - core) * n_chips + q, 1), :] = row_in[b, 0:1, :]
            with scope("wait_d2d"):
                theirs = mean_out.at[pl.ds(pl.multiple_of((1 - core) * half, half), half)]
                pltpu.make_async_remote_copy(
                    src_ref=theirs, dst_ref=theirs, send_sem=send_sem.at[FINAL_OUT], recv_sem=recv_sem.at[FINAL],
                    device_id=partner, device_id_type=MESH,
                ).wait_recv()
    with scope("drain"):
        for c in pending.values():
            c.wait_send()
        wait_group(X_OUT, x_all.at[1])
        wait_sums(sweeps - 1)
        wait_means(sweeps - 1)
        wait_group(FINAL_OUT, mean_out.at[pl.ds(0, half)])


def solution(mesh):
    n_pts, n_comp = mesh.shape["pts"], mesh.shape["comp"]
    n_chips = n_pts // CORES

    def per_device(points, means, log_w, inv_temp):
        n_loc, depth = points.shape
        k_loc = means.shape[0]
        kq = k_loc // n_pts
        half = n_chips * kq
        sweeps = inv_temp.shape[0]
        if n_chips != 4 or kq != LANES:
            raise ValueError("unsupported shape")
        f32, bf16 = jnp.float32, jnp.bfloat16
        kernel = functools.partial(
            em_kernel, sweeps, n_loc * n_pts, k_loc * n_comp, n_chips, n_comp
        )
        vmem = pl.BlockSpec(memory_space=pltpu.VMEM)
        hbm = pl.BlockSpec(memory_space=pltpu.HBM)
        V = pltpu.VMEM
        mean, logw, lse = pl.pallas_call(
            kernel,
            out_shape=(
                jax.ShapeDtypeStruct((k_loc, depth), f32),
                jax.ShapeDtypeStruct((n_pts, kq), f32),
                jax.ShapeDtypeStruct((n_loc // LANES, LANES), f32),
            ),
            in_specs=[hbm] * 4,
            out_specs=(vmem, vmem, vmem),
            scratch_shapes=[
                pltpu.SMEM((sweeps,), f32),
                V((n_pts, kq), f32),
                V((2, n_loc, depth), bf16),
                V((depth, 2 * n_loc), bf16),
                V((1, n_loc), f32),
                V((half, 2 * n_loc), f32),
                V((half, 2 * n_loc), bf16),
                V((4, kq, depth), f32),
                V((sweeps, 4, kq, depth), bf16),
                V((sweeps, 4, 8, kq), f32),
                V((4, 2 * n_loc), f32),
                V((4, 2 * n_loc), f32),
                V((4, 2 * n_loc), f32),
                V((sweeps, 2, n_loc), f32),
                V((sweeps, 2, n_loc), f32),
                V((sweeps, 2, n_loc), f32),
                V((sweeps, n_comp - 1, 2, n_loc), f32),
                V((sweeps, 1, n_loc), f32),
                V((sweeps, 1, n_loc), f32),
                V((4, kq, LANES), f32),
                V((half, min(256, n_loc)), f32),
                V((half, min(256, n_loc)), f32),
                V((2, 4, kq, LANES), f32),
                V((sweeps, 8, kq // 2, depth), f32),
                V((sweeps, 6, kq // 2, depth), f32),
                V((sweeps, 2, kq // 2, depth), f32),
                V((sweeps, 4, 8, kq), f32),
                V((sweeps, 3, 8, kq), f32),
                V((4, 8, kq), f32),
                V((4, 8, kq), f32),
                pltpu.SemaphoreType.DMA((SINGLE + 8 + n_comp,)),
                pltpu.SemaphoreType.DMA((ACROSS + sweeps * (n_comp - 1),)),
                pltpu.SemaphoreType.DMA((7,)),
            ],
            compiler_params=pltpu.CompilerParams(
                collective_id=0, has_side_effects=True, vmem_limit_bytes=44 * 1024 * 1024
            ),
            name="em",
        )(*(pltpu.with_memory_space_constraint(v, pltpu.HBM) for v in (inv_temp, points, means, log_w.reshape(n_pts, kq))))
        return mean, logw.reshape(k_loc), lse.reshape(n_loc)

    comp_spec = P(("fit", "comp"))
    return jax.shard_map(
        per_device,
        mesh=mesh,
        in_specs=(P(("fit", "pts"), None), P(("fit", "comp"), None), comp_spec, P()),
        out_specs=(P(("fit", "comp"), None), comp_spec, P(("fit", "pts"))),
        check_vma=False,
    )
```

```python
import contextlib
import functools
import math

import jax
import jax.numpy as jnp
from jax import lax
from jax.experimental import pallas as pl
from jax.experimental.pallas import tpu as pltpu
from jax.sharding import PartitionSpec as P

PRIOR_ALPHA = 1e-3
COUNT_EPS = 1e-6
LOG2E = math.log2(math.e)
LN2 = math.log(2.0)
MESH = pl.DeviceIdType.MESH
scope = contextlib.nullcontext
CORES = 2
PARTS = 4
DIRECT = 0
LANES = 128

OPP, RIGHT, LEFT, OWN = range(4)
SHIFT = {OPP: 2, RIGHT: 1, LEFT: 3, OWN: 0}

PAIR, SWAP, COUNT, ROW, FINAL, XPART, PIECES = 0, 1, 2, 5, 9, 10, 14
FAR_A, FAR_B, NEAR_A, NEAR_B, SUM_A, SUM_B, OWN_A_RIGHT, OWN_B_RIGHT, OWN_A_LEFT, OWN_B_LEFT, ON_A, ON_B = range(
    PIECES, PIECES + 12 * PARTS, PARTS
)
ACROSS = PIECES + 12 * PARTS
SUMS_RIGHT, SUMS_LEFT, MEANS_RIGHT, MEANS_LEFT, X_OUT, FINAL_OUT, SINGLE = range(7)


def em_kernel(
    sweeps, n_total, k_total, n_chips, n_comp,
    beta_hbm, x_hbm, mean_hbm, logw_hbm,
    mean_out, logw_out, lse_out,
    beta_ref, logw_ref, x_all, xt, x_sq, e_buf, r_buf, mean_f, mean_b, prm, m_st, s_st, factor, pair_out, pair_in, glob_out, glob_in,
    lse_own, lse_oth, cols_c, raw_0, raw_1, n_acc, s_buf, rs_in, acc_out, n_out, n_in, row_out, row_in, send_sem, recv_sem, copy_sem,
):
    raw = (raw_0, raw_1)
    n_loc, depth = x_all.shape[1], x_all.shape[2]
    kq = mean_f.shape[1]
    kh, kp = kq // 2, kq // 2 // PARTS
    half = n_chips * kq

    p = lax.axis_index("pts")
    y = lax.axis_index("comp")
    chip = lax.div(p, CORES)
    core = p - chip * CORES
    partner = {"pts": chip * CORES + 1 - core}

    def x_peer(d):
        return {"pts": lax.rem(chip + d, n_chips) * CORES + core}

    right, left, opposite = x_peer(1), x_peer(n_chips - 1), x_peer(2)
    y_order = sorted(range(1, n_comp), key=lambda d: -min(d, n_comp - d))
    y_peers = [{"comp": lax.rem(y + d, n_comp)} for d in y_order]

    barrier = pltpu.get_barrier_semaphore()
    everyone = [partner, right, left, opposite] + y_peers
    for dev in everyone:
        pl.semaphore_signal(barrier, inc=1, device_id=dev, device_id_type=MESH)

    tr = min(512, n_loc // 2)
    n_tr = n_loc // tr
    x_rows = [pl.ds(c * tr, tr) for c in range(n_tr)]
    load_x = [pltpu.make_async_copy(x_hbm.at[r], x_all.at[0, r], copy_sem.at[6 + c]) for c, r in enumerate(x_rows)]
    load_x[0].start()
    load_small = [
        pltpu.make_async_copy(logw_hbm, logw_ref, copy_sem.at[4]), pltpu.make_async_copy(beta_hbm, beta_ref, copy_sem.at[5])
    ]
    for c in load_small:
        c.start()
    load_mean = []
    for b in range(4):
        q = lax.rem(chip + SHIFT[b], n_chips)
        c = pltpu.make_async_copy(
            mean_hbm.at[pl.ds(pl.multiple_of(core * half + q * kq, kq), kq)], mean_f.at[b], copy_sem.at[b]
        )
        c.start()
        load_mean.append(c)

    for c in load_x[1:]:
        c.start()

    pending = {}

    def send(src, dst, arrive, depart, dev, when=None):
        c = pltpu.make_async_remote_copy(
            src_ref=src, dst_ref=dst, send_sem=send_sem.at[depart], recv_sem=recv_sem.at[arrive],
            device_id=dev, device_id_type=MESH,
        )
        if depart >= SINGLE:
            if depart in pending:
                pending[depart].wait_send()
            pending[depart] = c
        if when is None:
            c.start()
        else:
            pl.when(when)(c.start)
        return c

    def wait_group(depart, ref):
        pltpu.make_async_remote_copy(
            src_ref=ref, dst_ref=ref, send_sem=send_sem.at[depart], recv_sem=recv_sem.at[PAIR],
            device_id=partner, device_id_type=MESH,
        ).wait_send()

    def wait_sums(t):
        wait_group(SUMS_RIGHT, rs_in.at[t, pl.ds(0, 3)])
        wait_group(SUMS_LEFT, rs_in.at[t, pl.ds(0, 3)])

    def wait_means(t):
        ref = mean_b.at[t + 1, pl.ds(0, 3), pl.ds(0, kh)] if t < sweeps - 1 else mean_out.at[pl.ds(0, 3 * kh)]
        wait_group(MEANS_RIGHT, ref)
        wait_group(MEANS_LEFT, ref)

    eye = lax.broadcasted_iota(jnp.int32, (kq, kq), 0) == lax.broadcasted_iota(jnp.int32, (kq, kq), 1)

    def to_col(row):
        return jnp.sum(jnp.where(eye, jnp.broadcast_to(row, (kq, kq)), 0.0), axis=1, keepdims=True)

    def to_row(col):
        return jnp.sum(jnp.where(eye, jnp.broadcast_to(col, (kq, kq)), 0.0), axis=0, keepdims=True)

    with scope("barrier"):
        pl.semaphore_wait(barrier, len(everyone))
    x_copies = [send(x_hbm.at[r], x_all.at[1, r], XPART + c, X_OUT, partner) for c, r in enumerate(x_rows)]
    with scope("loads"):
        for c in load_small:
            c.wait()
    with scope("meanprep"):
        for b in range(4):
            load_mean[b].wait()
            mf = mean_f[b]
            mean_b[0, b] = mf.astype(jnp.bfloat16)
            q = lax.rem(chip + SHIFT[b], n_chips)
            prm[0, b, 0:1, :] = logw_ref[pl.ds(core * n_chips + q, 1), :]
            prm[0, b, 1:2, :] = to_row(jnp.sum(mf * mf, axis=1, keepdims=True))

    tile = min(256, n_loc // 2)

    def prepare(u):
        h, at = divmod(u * tile, n_loc)
        blk = x_all[h, at:at + tile, :].T
        xt[:, u * tile:(u + 1) * tile] = blk
        if h == 0:
            f = blk.astype(jnp.float32)
            x_sq[:, at:at + tile] = jnp.sum(f * f, axis=0, keepdims=True)

    def columns(t, blocks):
        for b in blocks:
            row = (prm[t, b, 0:1, :] - beta_ref[t] * prm[t, b, 1:2, :]) * LOG2E
            cols_c[b] = jnp.broadcast_to(to_col(row), (kq, LANES))

    def a_phase(t, tiles, blocks, ahead=None):
        slope = beta_ref[t] * (2.0 * LOG2E)
        lo, nb = blocks[0], len(blocks)
        means = mean_b.at[t, lo:lo + nb]

        def product(u):
            cols = slice(tiles[u] * tile, (tiles[u] + 1) * tile)
            raw[u % 2][0:nb * kq] = jnp.dot(
                means[...].reshape(nb * kq, depth), xt[:, cols], preferred_element_type=jnp.float32
            )

        if ahead is not None:
            ahead(tiles[0])
            ahead(tiles[1])
        product(0)
        for u in range(len(tiles)):
            if u + 1 < len(tiles):
                product(u + 1)
            if ahead is not None and u + 2 < len(tiles):
                ahead(tiles[u + 2])
            for v in range(tile // LANES):
                at = tiles[u] * tile + v * LANES
                cols = slice(at, at + LANES)
                for i, b in enumerate(blocks):
                    a = raw[u % 2][i * kq:(i + 1) * kq, v * LANES:(v + 1) * LANES]
                    logit = a * slope + cols_c[b]
                    m = jnp.max(logit, axis=0, keepdims=True)
                    e = jnp.exp2(logit - m)
                    e_buf[b * kq:(b + 1) * kq, cols] = e
                    m_st[b:b + 1, cols] = m
                    s_st[b:b + 1, cols] = jnp.sum(e, axis=0, keepdims=True)

    per_half = n_loc // tile
    tiles_of = [list(range(per_half)), list(range(per_half, 2 * per_half))]

    def local_pair(h):
        cols = pl.ds(h * n_loc, n_loc)
        ms = [m_st[b:b + 1, cols] for b in range(4)]
        m = jnp.maximum(jnp.maximum(ms[0], ms[1]), jnp.maximum(ms[2], ms[3]))
        s = sum(s_st[b:b + 1, cols] * jnp.exp2(ms[b] - m) for b in range(4))
        return m, s

    chunk = n_loc // 2

    def factors(h, lse):
        cols = slice(h * n_loc, (h + 1) * n_loc)
        factor[:, cols] = jnp.exp2(m_st[:, cols] - lse[...])

    def r_phase(h, lo, c):
        for b in (lo, lo + 1):
            acc = jnp.zeros((kq, LANES), jnp.float32)
            for at in range(h * n_loc + c * chunk, h * n_loc + (c + 1) * chunk, LANES):
                cols = slice(at, at + LANES)
                r = e_buf[b * kq:(b + 1) * kq, cols] * factor[b:b + 1, cols]
                r_buf[b * kq:(b + 1) * kq, cols] = r.astype(jnp.bfloat16)
                acc = acc + r
            n_acc[2 * h + c, b] = acc

    def stats(h, lo, c):
        at = h * n_loc + c * chunk
        out = jnp.dot(
            r_buf[lo * kq:(lo + 2) * kq, at:at + chunk], x_all[h, c * chunk:(c + 1) * chunk],
            preferred_element_type=jnp.float32,
        ).reshape(4, kh, depth)
        if h == 0 and c == 0:
            s_buf[t, 2 * lo:2 * lo + 4] = out
        else:
            s_buf[t, 2 * lo:2 * lo + 4] += out

    for t in range(sweeps):
        last = t == sweeps - 1
        if t == 0:
            columns(0, range(4))
            with scope("loadx"):
                for c in load_x:
                    c.wait()
            with scope("a00"):
                a_phase(t, tiles_of[0], range(4), prepare)
            for g in range(2):
                with scope("xwait"):
                    for c in x_copies[g * n_tr // 2:(g + 1) * n_tr // 2]:
                        c.wait_recv()
                with scope("a01"):
                    a_phase(t, tiles_of[1][g * per_half // 2:(g + 1) * per_half // 2], range(4), prepare)
        else:
            with scope("wait_near"):
                for c in b_right + a_left + rows[:2]:
                    c.wait_recv()
            with scope("a_right"):
                columns(t, (RIGHT, LEFT))
                a_phase(t, tiles_of[1] + tiles_of[0], (RIGHT, LEFT))
            with scope("wait_opp"):
                for c in a_on + b_on + rows[2:]:
                    c.wait_recv()
            with scope("a_opp1"):
                columns(t, (OPP,))
                a_phase(t, tiles_of[1], (OPP,))
        m, s = local_pair(1)
        pair_out[t, 0:1, :] = m
        pair_out[t, 1:2, :] = s
        pair = send(pair_out.at[t], pair_in.at[t], PAIR, SINGLE, partner)
        if t > 0:
            with scope("a_opp0"):
                a_phase(t, tiles_of[0], (OPP,))
        m, s = local_pair(0)
        with scope("wait_pair"):
            pair.wait_recv()
        m1, s1 = pair_in[t, 0:1, :], pair_in[t, 1:2, :]
        top = jnp.maximum(m, m1)
        s = s * jnp.exp2(m - top) + s1 * jnp.exp2(m1 - top)
        glob_out[t, 0:1, :] = top
        glob_out[t, 1:2, :] = s
        across = [
            send(glob_out.at[t], glob_in.at[t, d], ACROSS + t * (n_comp - 1) + d, SINGLE + 9 + d, y_peers[d])
            for d in range(n_comp - 1)
        ]
        tops, sums = [top], [s]
        for d in reversed(range(n_comp - 1)):
            with scope("wait_y"):
                across[d].wait_recv()
            tops.append(glob_in[t, d, 0:1, :])
            sums.append(glob_in[t, d, 1:2, :])
        top = functools.reduce(jnp.maximum, tops)
        total = sum(v * jnp.exp2(w - top) for v, w in zip(sums, tops))
        lse2 = top + jnp.log(total) * LOG2E
        lse_own[t] = lse2
        swap = send(lse_own.at[t], lse_oth.at[t], SWAP, SINGLE + 1, partner)
        if last:
            lse = lse2 * LN2 - beta_ref[t] * x_sq[...]
            for i in range(n_loc // LANES):
                lse_out[i:i + 1, :] = lse[:, i * LANES:(i + 1) * LANES]

        with scope("rs_own"):
            factors(0, lse_own.at[t])
            r_phase(0, 0, 0)
            r_phase(0, 0, 1)
            stats(0, 0, 0)
        with scope("wait_swap"):
            swap.wait_recv()
        with scope("stats1"):
            factors(1, lse_oth.at[t])
            r_phase(1, 0, 0)
            stats(0, 0, 1)
            r_phase(1, 0, 1)
            stats(1, 0, 0)
            stats(1, 0, 1)

        parts = [pl.ds(i * kp, kp) for i in range(PARTS)]

        def s_piece(b, half_b, i):
            return s_buf.at[t, 2 * b + half_b, parts[i]]

        def in_piece(slot, i):
            return rs_in.at[t, slot, parts[i]]

        def near_b_send(i, when=None):
            return send(s_piece(RIGHT, 1, i), in_piece(2, i), NEAR_B + i, SUMS_RIGHT, right, when)

        def near_a_send(i):
            return send(s_piece(LEFT, 0, i), in_piece(3, i), NEAR_A + i, SUMS_LEFT, left)

        def first_sends(when):
            a, b = [], []
            for i in range(PARTS):
                a.append(send(s_piece(OPP, 0, i), in_piece(0, i), FAR_A + i, SUMS_RIGHT, right, when))
                b.append(send(s_piece(OPP, 1, i), in_piece(1, i), FAR_B + i, SUMS_LEFT, left, when))
            return a, b, [near_b_send(i, when) for i in range(2)]

        if t > 0:
            wait_sums(t - 1)
        far_a, far_b, near_b = first_sends(core == 0)
        with scope("r_23"):
            for h in range(2):
                for c in range(2):
                    r_phase(h, 2, c)
        counts = []
        for b in range(4):
            row = to_row(jnp.sum((n_acc[0, b] + n_acc[1, b]) + (n_acc[2, b] + n_acc[3, b]), axis=1, keepdims=True))
            n_out[t, b, 0:1, :] = row
            counts.append(row)
        n_copies = [
            send(n_out.at[t, b], n_in.at[t, d], COUNT + d, SINGLE + 2 + d, dev)
            for d, (b, dev) in enumerate(((OPP, opposite), (RIGHT, right), (LEFT, left)))
        ]
        with scope("stats2"):
            for h in range(2):
                for c in range(2):
                    stats(h, 2, c)
        first_sends(core == 1)
        near_a = [near_a_send(i) for i in range(2)]
        sum_a, sum_b = [], []
        for i in range(PARTS):
            with scope("wait_far_a"):
                far_a[i].wait_recv()
            acc_out[t, 0, parts[i]] = s_buf[t, 2 * RIGHT, parts[i]] + rs_in[t, 0, parts[i]]
            sum_a.append(send(acc_out.at[t, 0, parts[i]], in_piece(4, i), SUM_A + i, SUMS_RIGHT, right))
            if i + 2 < PARTS:
                near_b.append(near_b_send(i + 2))
            with scope("wait_far_b"):
                far_b[i].wait_recv()
            acc_out[t, 1, parts[i]] = s_buf[t, 2 * LEFT + 1, parts[i]] + rs_in[t, 1, parts[i]]
            sum_b.append(send(acc_out.at[t, 1, parts[i]], in_piece(5, i), SUM_B + i, SUMS_LEFT, left))
            if i + 2 < PARTS:
                near_a.append(near_a_send(i + 2))

        n_row = counts[OWN]
        for d in range(3):
            with scope("wait_n"):
                n_copies[d].wait_recv()
            n_row = n_row + n_in[t, d, 0:1, :]
        n_col = to_col(n_row) + COUNT_EPS
        logw = jnp.log((n_row + PRIOR_ALPHA) / (n_total + k_total * PRIOR_ALPHA))

        def m_piece(b, half_b, i):
            at = half_b * kh + i * kp
            if not last:
                return mean_b.at[t + 1, b, pl.ds(at, kp)]
            q = lax.rem(chip + SHIFT[b], n_chips)
            return mean_out.at[pl.ds(pl.multiple_of(core * half + q * kq + at, kp), kp)]

        def m_send(b, there, half_b, i, arrive, dev):
            depart = MEANS_LEFT if arrive >= OWN_A_LEFT and not ON_A <= arrive < ON_B else MEANS_RIGHT
            return send(m_piece(b, half_b, i), m_piece(b if last else there, half_b, i), arrive, depart, dev)

        def swap_piece(b, half_b, i):
            if last:
                send(m_piece(b, half_b, i), m_piece(b, half_b, i), FINAL, FINAL_OUT, partner)

        rows = []

        def send_rows(mean_sq=None):
            own_row, to_rows = (row_out.at[OWN], row_out) if last else (prm.at[t + 1, OWN], prm.at[t + 1])
            own_row[0:1, :] = logw
            if mean_sq is not None:
                own_row[1:2, :] = mean_sq
            for d, (b, dev) in enumerate(((LEFT, right), (RIGHT, left), (OPP, opposite))):
                rows.append(send(own_row, to_rows.at[b], ROW + d, SINGLE + 5 + d, dev))

        if t > 0:
            wait_means(t - 1)
        if last:
            send_rows()
        sq = {}
        a_right, b_right, a_left, b_left, a_on, b_on, a_direct, b_direct = ([] for _ in range(8))
        for i in range(PARTS):
            for half_b, far, near, slots in ((0, sum_a, near_a, (3, 4)), (1, sum_b, near_b, (2, 5))):
                with scope("wait_sum"):
                    near[i].wait_recv()
                    far[i].wait_recv()
                at = half_b * kh + i * kp
                mean = (
                    s_buf[t, 2 * OWN + half_b, parts[i]] + rs_in[t, slots[0], parts[i]] + rs_in[t, slots[1], parts[i]]
                ) / n_col[at:at + kp]
                m_piece(OWN, half_b, i)[...] = mean if last else mean.astype(jnp.bfloat16)
                sq[half_b, i] = jnp.sum(mean * mean, axis=1, keepdims=True)
                if half_b == 0:
                    a_right.append(m_send(OWN, LEFT, 0, i, OWN_A_RIGHT + i, right))
                else:
                    b_left.append(m_send(OWN, RIGHT, 1, i, OWN_B_LEFT + i, left))
            b_right.append(m_send(OWN, LEFT, 1, i, OWN_B_RIGHT + i, right))
            a_left.append(m_send(OWN, RIGHT, 0, i, OWN_A_LEFT + i, left))
            if i >= PARTS - DIRECT:
                a_direct.append(m_send(OWN, OPP, 0, i, ON_A + i, opposite))
                b_direct.append(m_send(OWN, OPP, 1, i, ON_B + i, opposite))
            swap_piece(OWN, 0, i)
            swap_piece(OWN, 1, i)

        if not last:
            send_rows(to_row(jnp.concatenate([sq[h, i] for h in range(2) for i in range(PARTS)], axis=0)))
        if not last:
            with scope("a_own"):
                columns(t + 1, (OWN,))
                a_phase(t + 1, tiles_of[1] + tiles_of[0], (OWN,))
        for i in range(PARTS):
            with scope("wait_on_a"):
                a_right[i].wait_recv()
            if i < PARTS - DIRECT:
                a_on.append(m_send(LEFT, OPP, 0, i, ON_A + i, right))
            with scope("wait_on_b"):
                b_left[i].wait_recv()
            if i < PARTS - DIRECT:
                b_on.append(m_send(RIGHT, OPP, 1, i, ON_B + i, left))
            swap_piece(LEFT, 0, i)
            swap_piece(RIGHT, 1, i)
        a_on += a_direct
        b_on += b_direct
        if last:
            with scope("wait_rows"):
                for c in rows:
                    c.wait_recv()
            rows_copy = send(row_out, row_in, ROW + 3, SINGLE + 8, partner)
            for i in range(PARTS):
                with scope("wait_bl"):
                    b_right[i].wait_recv()
                swap_piece(LEFT, 1, i)
                with scope("wait_ar"):
                    a_left[i].wait_recv()
                swap_piece(RIGHT, 0, i)
            for i in range(PARTS):
                with scope("wait_oa"):
                    a_on[i].wait_recv()
                swap_piece(OPP, 0, i)
                with scope("wait_ob"):
                    b_on[i].wait_recv()
                swap_piece(OPP, 1, i)
            with scope("wait_d2dr"):
                rows_copy.wait_recv()
            for b in range(4):
                q = lax.rem(chip + SHIFT[b], n_chips)
                logw_out[pl.ds(core * n_chips + q, 1), :] = row_out[b, 0:1, :]
                logw_out[pl.ds((1 - core) * n_chips + q, 1), :] = row_in[b, 0:1, :]
            with scope("wait_d2d"):
                theirs = mean_out.at[pl.ds(pl.multiple_of((1 - core) * half, half), half)]
                pltpu.make_async_remote_copy(
                    src_ref=theirs, dst_ref=theirs, send_sem=send_sem.at[FINAL_OUT], recv_sem=recv_sem.at[FINAL],
                    device_id=partner, device_id_type=MESH,
                ).wait_recv()
    with scope("drain"):
        for c in pending.values():
            c.wait_send()
        wait_group(X_OUT, x_all.at[1])
        wait_sums(sweeps - 1)
        wait_means(sweeps - 1)
        wait_group(FINAL_OUT, mean_out.at[pl.ds(0, half)])


def pass_kernel(mean_in, logw_in, lse_in, mean_out, logw_out, lse_out, sem):
    copies = [
        pltpu.make_async_copy(src, dst, sem.at[i])
        for i, (src, dst) in enumerate(((mean_in, mean_out), (logw_in, logw_out), (lse_in, lse_out)))
    ]
    for c in copies:
        c.start()
    for c in copies:
        c.wait()


def solution(mesh):
    n_pts, n_comp = mesh.shape["pts"], mesh.shape["comp"]
    n_chips = n_pts // CORES

    def per_device(points, means, log_w, inv_temp):
        n_loc, depth = points.shape
        k_loc = means.shape[0]
        kq = k_loc // n_pts
        half = n_chips * kq
        sweeps = inv_temp.shape[0]
        if n_chips != 4 or kq != LANES:
            raise ValueError("unsupported shape")
        f32, bf16 = jnp.float32, jnp.bfloat16
        kernel = functools.partial(
            em_kernel, sweeps, n_loc * n_pts, k_loc * n_comp, n_chips, n_comp
        )
        vmem = pl.BlockSpec(memory_space=pltpu.VMEM)
        hbm = pl.BlockSpec(memory_space=pltpu.HBM)
        V = pltpu.VMEM
        mean, logw, lse = pl.pallas_call(
            kernel,
            out_shape=(
                jax.ShapeDtypeStruct((k_loc, depth), f32),
                jax.ShapeDtypeStruct((n_pts, kq), f32),
                jax.ShapeDtypeStruct((n_loc // LANES, LANES), f32),
            ),
            in_specs=[hbm] * 4,
            out_specs=(vmem, vmem, vmem),
            scratch_shapes=[
                pltpu.SMEM((sweeps,), f32),
                V((n_pts, kq), f32),
                V((2, n_loc, depth), bf16),
                V((depth, 2 * n_loc), bf16),
                V((1, n_loc), f32),
                V((half, 2 * n_loc), f32),
                V((half, 2 * n_loc), bf16),
                V((4, kq, depth), f32),
                V((sweeps, 4, kq, depth), bf16),
                V((sweeps, 4, 8, kq), f32),
                V((4, 2 * n_loc), f32),
                V((4, 2 * n_loc), f32),
                V((4, 2 * n_loc), f32),
                V((sweeps, 2, n_loc), f32),
                V((sweeps, 2, n_loc), f32),
                V((sweeps, 2, n_loc), f32),
                V((sweeps, n_comp - 1, 2, n_loc), f32),
                V((sweeps, 1, n_loc), f32),
                V((sweeps, 1, n_loc), f32),
                V((4, kq, LANES), f32),
                V((half, min(256, n_loc // 2)), f32),
                V((half, min(256, n_loc // 2)), f32),
                V((4, 4, kq, LANES), f32),
                V((sweeps, 8, kq // 2, depth), f32),
                V((sweeps, 6, kq // 2, depth), f32),
                V((sweeps, 2, kq // 2, depth), f32),
                V((sweeps, 4, 8, kq), f32),
                V((sweeps, 3, 8, kq), f32),
                V((4, 8, kq), f32),
                V((4, 8, kq), f32),
                pltpu.SemaphoreType.DMA((SINGLE + 8 + n_comp,)),
                pltpu.SemaphoreType.DMA((ACROSS + sweeps * (n_comp - 1),)),
                pltpu.SemaphoreType.DMA((10,)),
            ],
            compiler_params=pltpu.CompilerParams(
                collective_id=0, has_side_effects=True, vmem_limit_bytes=44 * 1024 * 1024
            ),
            name="em",
        )(*(pltpu.with_memory_space_constraint(v, pltpu.HBM) for v in (inv_temp, points, means, log_w.reshape(n_pts, kq))))
        copies = (mean, logw, lse)
        mean, logw, lse = pl.pallas_call(
            pass_kernel,
            out_shape=tuple(pltpu.HBM(v.shape, f32) for v in copies),
            in_specs=[vmem] * 3,
            out_specs=(hbm,) * 3,
            scratch_shapes=[pltpu.SemaphoreType.DMA((3,))],
            name="results",
        )(*(pltpu.with_memory_space_constraint(v, pltpu.VMEM) for v in copies))
        return mean, logw.reshape(k_loc), lse.reshape(n_loc)

    comp_spec = P(("fit", "comp"))
    return jax.shard_map(
        per_device,
        mesh=mesh,
        in_specs=(P(("fit", "pts"), None), P(("fit", "comp"), None), comp_spec, P()),
        out_specs=(P(("fit", "comp"), None), comp_spec, P(("fit", "pts"))),
        check_vma=False,
    )
```

```python
import contextlib
import functools
import math

import jax
import jax.numpy as jnp
from jax import lax
from jax.experimental import pallas as pl
from jax.experimental.pallas import tpu as pltpu
from jax.sharding import PartitionSpec as P

PRIOR_ALPHA = 1e-3
COUNT_EPS = 1e-6
LOG2E = math.log2(math.e)
LN2 = math.log(2.0)
MESH = pl.DeviceIdType.MESH
scope = contextlib.nullcontext
CORES = 2
PARTS = 2
DIRECT = 0
LANES = 128

OPP, RIGHT, LEFT, OWN = range(4)
SHIFT = {OPP: 2, RIGHT: 1, LEFT: 3, OWN: 0}

PAIR, SWAP, COUNT, ROW, FINAL, XPART, PIECES = 0, 1, 2, 5, 9, 10, 14
FAR_A, FAR_B, NEAR_A, NEAR_B, SUM_A, SUM_B, OWN_A_RIGHT, OWN_B_RIGHT, OWN_A_LEFT, OWN_B_LEFT, ON_A, ON_B = range(
    PIECES, PIECES + 12 * PARTS, PARTS
)
ACROSS = PIECES + 12 * PARTS
SUMS_RIGHT, SUMS_LEFT, MEANS_RIGHT, MEANS_LEFT, X_OUT, FINAL_OUT, SINGLE = range(7)


def em_kernel(
    sweeps, n_total, k_total, n_chips, n_comp,
    beta_hbm, x_hbm, mean_hbm, logw_hbm,
    mean_out, logw_out, lse_out,
    beta_ref, logw_ref, x_all, xt, x_sq, e_buf, r_buf, mean_f, mean_b, prm, m_st, s_st, factor, pair_out, pair_in, glob_out, glob_in,
    lse_own, lse_oth, cols_c, raw_0, raw_1, n_acc, s_buf, rs_in, acc_out, n_out, n_in, row_out, row_in, send_sem, recv_sem, copy_sem,
):
    raw = (raw_0, raw_1)
    n_loc, depth = x_all.shape[1], x_all.shape[2]
    kq = mean_f.shape[1]
    kh, kp = kq // 2, kq // 2 // PARTS
    half = n_chips * kq

    p = lax.axis_index("pts")
    y = lax.axis_index("comp")
    chip = lax.div(p, CORES)
    core = p - chip * CORES
    partner = {"pts": chip * CORES + 1 - core}

    def x_peer(d):
        return {"pts": lax.rem(chip + d, n_chips) * CORES + core}

    right, left, opposite = x_peer(1), x_peer(n_chips - 1), x_peer(2)
    y_order = sorted(range(1, n_comp), key=lambda d: -min(d, n_comp - d))
    y_peers = [{"comp": lax.rem(y + d, n_comp)} for d in y_order]

    barrier = pltpu.get_barrier_semaphore()
    everyone = [partner, right, left, opposite] + y_peers
    for dev in everyone:
        pl.semaphore_signal(barrier, inc=1, device_id=dev, device_id_type=MESH)

    tr = min(512, n_loc // 2)
    n_tr = n_loc // tr
    x_rows = [pl.ds(c * tr, tr) for c in range(n_tr)]
    load_x = [pltpu.make_async_copy(x_hbm.at[r], x_all.at[0, r], copy_sem.at[6 + c]) for c, r in enumerate(x_rows)]
    load_x[0].start()
    load_small = [
        pltpu.make_async_copy(logw_hbm, logw_ref, copy_sem.at[4]), pltpu.make_async_copy(beta_hbm, beta_ref, copy_sem.at[5])
    ]
    for c in load_small:
        c.start()
    load_mean = []
    for b in range(4):
        q = lax.rem(chip + SHIFT[b], n_chips)
        c = pltpu.make_async_copy(
            mean_hbm.at[pl.ds(pl.multiple_of(core * half + q * kq, kq), kq)], mean_f.at[b], copy_sem.at[b]
        )
        c.start()
        load_mean.append(c)

    for c in load_x[1:]:
        c.start()

    pending = {}

    def send(src, dst, arrive, depart, dev, when=None):
        c = pltpu.make_async_remote_copy(
            src_ref=src, dst_ref=dst, send_sem=send_sem.at[depart], recv_sem=recv_sem.at[arrive],
            device_id=dev, device_id_type=MESH,
        )
        if depart >= SINGLE:
            if depart in pending:
                pending[depart].wait_send()
            pending[depart] = c
        if when is None:
            c.start()
        else:
            pl.when(when)(c.start)
        return c

    def wait_group(depart, ref):
        pltpu.make_async_remote_copy(
            src_ref=ref, dst_ref=ref, send_sem=send_sem.at[depart], recv_sem=recv_sem.at[PAIR],
            device_id=partner, device_id_type=MESH,
        ).wait_send()

    def wait_sums(t):
        wait_group(SUMS_RIGHT, rs_in.at[t, pl.ds(0, 3)])
        wait_group(SUMS_LEFT, rs_in.at[t, pl.ds(0, 3)])

    def wait_means(t):
        ref = mean_b.at[t + 1, pl.ds(0, 3), pl.ds(0, kh)] if t < sweeps - 1 else mean_out.at[pl.ds(0, 3 * kh)]
        wait_group(MEANS_RIGHT, ref)
        wait_group(MEANS_LEFT, ref)

    eye = lax.broadcasted_iota(jnp.int32, (kq, kq), 0) == lax.broadcasted_iota(jnp.int32, (kq, kq), 1)

    def to_col(row):
        return jnp.sum(jnp.where(eye, jnp.broadcast_to(row, (kq, kq)), 0.0), axis=1, keepdims=True)

    def to_row(col):
        return jnp.sum(jnp.where(eye, jnp.broadcast_to(col, (kq, kq)), 0.0), axis=0, keepdims=True)

    with scope("barrier"):
        pl.semaphore_wait(barrier, len(everyone))
    x_copies = [send(x_hbm.at[r], x_all.at[1, r], XPART + c, X_OUT, partner) for c, r in enumerate(x_rows)]
    with scope("loads"):
        for c in load_small:
            c.wait()
    with scope("meanprep"):
        for b in range(4):
            load_mean[b].wait()
            mf = mean_f[b]
            mean_b[0, b] = mf.astype(jnp.bfloat16)
            q = lax.rem(chip + SHIFT[b], n_chips)
            prm[0, b, 0:1, :] = logw_ref[pl.ds(core * n_chips + q, 1), :]
            prm[0, b, 1:2, :] = to_row(jnp.sum(mf * mf, axis=1, keepdims=True))

    tile = min(256, n_loc // 2)

    def prepare(u):
        h, at = divmod(u * tile, n_loc)
        blk = x_all[h, at:at + tile, :].T
        xt[:, u * tile:(u + 1) * tile] = blk
        if h == 0:
            f = blk.astype(jnp.float32)
            x_sq[:, at:at + tile] = jnp.sum(f * f, axis=0, keepdims=True)

    def columns(t, blocks):
        for b in blocks:
            row = (prm[t, b, 0:1, :] - beta_ref[t] * prm[t, b, 1:2, :]) * LOG2E
            cols_c[b] = jnp.broadcast_to(to_col(row), (kq, LANES))

    def a_phase(t, tiles, blocks, ahead=None):
        slope = beta_ref[t] * (2.0 * LOG2E)
        lo, nb = blocks[0], len(blocks)
        means = mean_b.at[t, lo:lo + nb]

        def product(u):
            cols = slice(tiles[u] * tile, (tiles[u] + 1) * tile)
            raw[u % 2][0:nb * kq] = jnp.dot(
                means[...].reshape(nb * kq, depth), xt[:, cols], preferred_element_type=jnp.float32
            )

        if ahead is not None:
            ahead(tiles[0])
            ahead(tiles[1])
        product(0)
        for u in range(len(tiles)):
            if u + 1 < len(tiles):
                product(u + 1)
            if ahead is not None and u + 2 < len(tiles):
                ahead(tiles[u + 2])
            for v in range(tile // LANES):
                at = tiles[u] * tile + v * LANES
                cols = slice(at, at + LANES)
                for i, b in enumerate(blocks):
                    a = raw[u % 2][i * kq:(i + 1) * kq, v * LANES:(v + 1) * LANES]
                    logit = a * slope + cols_c[b]
                    m = jnp.max(logit, axis=0, keepdims=True)
                    e = jnp.exp2(logit - m)
                    e_buf[b * kq:(b + 1) * kq, cols] = e
                    m_st[b:b + 1, cols] = m
                    s_st[b:b + 1, cols] = jnp.sum(e, axis=0, keepdims=True)

    per_half = n_loc // tile
    tiles_of = [list(range(per_half)), list(range(per_half, 2 * per_half))]

    def local_pair(h):
        cols = pl.ds(h * n_loc, n_loc)
        ms = [m_st[b:b + 1, cols] for b in range(4)]
        m = jnp.maximum(jnp.maximum(ms[0], ms[1]), jnp.maximum(ms[2], ms[3]))
        s = sum(s_st[b:b + 1, cols] * jnp.exp2(ms[b] - m) for b in range(4))
        return m, s

    def r_phase(h, blocks, lse):
        half_cols = slice(h * n_loc, (h + 1) * n_loc)
        if 0 in blocks:
            factor[:, half_cols] = jnp.exp2(m_st[:, half_cols] - lse[...])
        accs = [jnp.zeros((kq, LANES), jnp.float32) for _ in blocks]
        for c in range(n_loc // LANES):
            cols = slice(h * n_loc + c * LANES, h * n_loc + (c + 1) * LANES)
            for i, b in enumerate(blocks):
                r = e_buf[b * kq:(b + 1) * kq, cols] * factor[b:b + 1, cols]
                r_buf[b * kq:(b + 1) * kq, cols] = r.astype(jnp.bfloat16)
                accs[i] = accs[i] + r
        for i, b in enumerate(blocks):
            n_acc[h, b] = accs[i]

    def stats(h, lo):
        out = jnp.dot(
            r_buf[lo * kq:(lo + 2) * kq, h * n_loc:(h + 1) * n_loc], x_all[h], preferred_element_type=jnp.float32
        ).reshape(4, kh, depth)
        if h == 0:
            s_buf[t, 2 * lo:2 * lo + 4] = out
        else:
            s_buf[t, 2 * lo:2 * lo + 4] += out

    for t in range(sweeps):
        last = t == sweeps - 1
        if t == 0:
            columns(0, range(4))
            with scope("loadx"):
                for c in load_x:
                    c.wait()
            with scope("a00"):
                a_phase(t, tiles_of[0], range(4), prepare)
            for g in range(2):
                with scope("xwait"):
                    for c in x_copies[g * n_tr // 2:(g + 1) * n_tr // 2]:
                        c.wait_recv()
                with scope("a01"):
                    a_phase(t, tiles_of[1][g * per_half // 2:(g + 1) * per_half // 2], range(4), prepare)
        else:
            with scope("wait_near"):
                for c in b_right + a_left + rows[:2]:
                    c.wait_recv()
            with scope("a_right"):
                columns(t, (RIGHT, LEFT))
                a_phase(t, tiles_of[1] + tiles_of[0], (RIGHT, LEFT))
            with scope("wait_opp"):
                for c in a_on + b_on + rows[2:]:
                    c.wait_recv()
            with scope("a_opp1"):
                columns(t, (OPP,))
                a_phase(t, tiles_of[1], (OPP,))
        m, s = local_pair(1)
        pair_out[t, 0:1, :] = m
        pair_out[t, 1:2, :] = s
        pair = send(pair_out.at[t], pair_in.at[t], PAIR, SINGLE, partner)
        if t > 0:
            with scope("a_opp0"):
                a_phase(t, tiles_of[0], (OPP,))
        m, s = local_pair(0)
        with scope("wait_pair"):
            pair.wait_recv()
        m1, s1 = pair_in[t, 0:1, :], pair_in[t, 1:2, :]
        top = jnp.maximum(m, m1)
        s = s * jnp.exp2(m - top) + s1 * jnp.exp2(m1 - top)
        glob_out[t, 0:1, :] = top
        glob_out[t, 1:2, :] = s
        across = [
            send(glob_out.at[t], glob_in.at[t, d], ACROSS + t * (n_comp - 1) + d, SINGLE + 9 + d, y_peers[d])
            for d in range(n_comp - 1)
        ]
        tops, sums = [top], [s]
        for d in reversed(range(n_comp - 1)):
            with scope("wait_y"):
                across[d].wait_recv()
            tops.append(glob_in[t, d, 0:1, :])
            sums.append(glob_in[t, d, 1:2, :])
        top = functools.reduce(jnp.maximum, tops)
        total = sum(v * jnp.exp2(w - top) for v, w in zip(sums, tops))
        lse2 = top + jnp.log(total) * LOG2E
        lse_own[t] = lse2
        swap = send(lse_own.at[t], lse_oth.at[t], SWAP, SINGLE + 1, partner)
        if last:
            lse = lse2 * LN2 - beta_ref[t] * x_sq[...]
            for i in range(n_loc // LANES):
                lse_out[i:i + 1, :] = lse[:, i * LANES:(i + 1) * LANES]

        own_r, oth_r = lse_own.at[t], lse_oth.at[t]
        with scope("r_own_a"):
            r_phase(0, (0, 1), own_r)
        with scope("stats0"):
            stats(0, 0)
        with scope("wait_swap"):
            swap.wait_recv()
        with scope("r_oth_a"):
            r_phase(1, (0, 1), oth_r)
        with scope("stats1"):
            stats(1, 0)

        parts = [pl.ds(i * kp, kp) for i in range(PARTS)]

        def s_piece(b, half_b, i):
            return s_buf.at[t, 2 * b + half_b, parts[i]]

        def in_piece(slot, i):
            return rs_in.at[t, slot, parts[i]]

        def near_b_send(i, when=None):
            return send(s_piece(RIGHT, 1, i), in_piece(2, i), NEAR_B + i, SUMS_RIGHT, right, when)

        def near_a_send(i):
            return send(s_piece(LEFT, 0, i), in_piece(3, i), NEAR_A + i, SUMS_LEFT, left)

        def first_sends(when):
            a, b = [], []
            for i in range(PARTS):
                a.append(send(s_piece(OPP, 0, i), in_piece(0, i), FAR_A + i, SUMS_RIGHT, right, when))
                b.append(send(s_piece(OPP, 1, i), in_piece(1, i), FAR_B + i, SUMS_LEFT, left, when))
            return a, b, [near_b_send(i, when) for i in range(2)]

        if t > 0:
            wait_sums(t - 1)
        far_a, far_b, near_b = first_sends(core == 0)
        with scope("r_23"):
            r_phase(0, (2, 3), own_r)
            r_phase(1, (2, 3), oth_r)
        counts = []
        for b in range(4):
            row = to_row(jnp.sum(n_acc[0, b] + n_acc[1, b], axis=1, keepdims=True))
            n_out[t, b, 0:1, :] = row
            counts.append(row)
        n_copies = [
            send(n_out.at[t, b], n_in.at[t, d], COUNT + d, SINGLE + 2 + d, dev)
            for d, (b, dev) in enumerate(((OPP, opposite), (RIGHT, right), (LEFT, left)))
        ]
        with scope("stats2"):
            stats(0, 2)
            stats(1, 2)
        first_sends(core == 1)
        near_a = [near_a_send(i) for i in range(2)]
        sum_a, sum_b = [], []
        for i in range(PARTS):
            with scope("wait_far_a"):
                far_a[i].wait_recv()
            acc_out[t, 0, parts[i]] = s_buf[t, 2 * RIGHT, parts[i]] + rs_in[t, 0, parts[i]]
            sum_a.append(send(acc_out.at[t, 0, parts[i]], in_piece(4, i), SUM_A + i, SUMS_RIGHT, right))
            if i + 2 < PARTS:
                near_b.append(near_b_send(i + 2))
            with scope("wait_far_b"):
                far_b[i].wait_recv()
            acc_out[t, 1, parts[i]] = s_buf[t, 2 * LEFT + 1, parts[i]] + rs_in[t, 1, parts[i]]
            sum_b.append(send(acc_out.at[t, 1, parts[i]], in_piece(5, i), SUM_B + i, SUMS_LEFT, left))
            if i + 2 < PARTS:
                near_a.append(near_a_send(i + 2))

        n_row = counts[OWN]
        for d in range(3):
            with scope("wait_n"):
                n_copies[d].wait_recv()
            n_row = n_row + n_in[t, d, 0:1, :]
        n_col = to_col(n_row) + COUNT_EPS
        logw = jnp.log((n_row + PRIOR_ALPHA) / (n_total + k_total * PRIOR_ALPHA))

        def m_piece(b, half_b, i):
            at = half_b * kh + i * kp
            if not last:
                return mean_b.at[t + 1, b, pl.ds(at, kp)]
            q = lax.rem(chip + SHIFT[b], n_chips)
            return mean_out.at[pl.ds(pl.multiple_of(core * half + q * kq + at, kp), kp)]

        def m_send(b, there, half_b, i, arrive, dev):
            depart = MEANS_LEFT if arrive >= OWN_A_LEFT and not ON_A <= arrive < ON_B else MEANS_RIGHT
            return send(m_piece(b, half_b, i), m_piece(b if last else there, half_b, i), arrive, depart, dev)

        def swap_piece(b, half_b, i):
            if last:
                send(m_piece(b, half_b, i), m_piece(b, half_b, i), FINAL, FINAL_OUT, partner)

        rows = []

        def send_rows(mean_sq=None):
            own_row, to_rows = (row_out.at[OWN], row_out) if last else (prm.at[t + 1, OWN], prm.at[t + 1])
            own_row[0:1, :] = logw
            if mean_sq is not None:
                own_row[1:2, :] = mean_sq
            for d, (b, dev) in enumerate(((LEFT, right), (RIGHT, left), (OPP, opposite))):
                rows.append(send(own_row, to_rows.at[b], ROW + d, SINGLE + 5 + d, dev))

        if t > 0:
            wait_means(t - 1)
        if last:
            send_rows()
        sq = {}
        a_right, b_right, a_left, b_left, a_on, b_on, a_direct, b_direct = ([] for _ in range(8))
        for i in range(PARTS):
            for half_b, far, near, slots in ((0, sum_a, near_a, (3, 4)), (1, sum_b, near_b, (2, 5))):
                with scope("wait_sum"):
                    near[i].wait_recv()
                    far[i].wait_recv()
                at = half_b * kh + i * kp
                mean = (
                    s_buf[t, 2 * OWN + half_b, parts[i]] + rs_in[t, slots[0], parts[i]] + rs_in[t, slots[1], parts[i]]
                ) / n_col[at:at + kp]
                m_piece(OWN, half_b, i)[...] = mean if last else mean.astype(jnp.bfloat16)
                sq[half_b, i] = jnp.sum(mean * mean, axis=1, keepdims=True)
                if half_b == 0:
                    a_right.append(m_send(OWN, LEFT, 0, i, OWN_A_RIGHT + i, right))
                else:
                    b_left.append(m_send(OWN, RIGHT, 1, i, OWN_B_LEFT + i, left))
            b_right.append(m_send(OWN, LEFT, 1, i, OWN_B_RIGHT + i, right))
            a_left.append(m_send(OWN, RIGHT, 0, i, OWN_A_LEFT + i, left))
            if i >= PARTS - DIRECT:
                a_direct.append(m_send(OWN, OPP, 0, i, ON_A + i, opposite))
                b_direct.append(m_send(OWN, OPP, 1, i, ON_B + i, opposite))
            swap_piece(OWN, 0, i)
            swap_piece(OWN, 1, i)

        if not last:
            send_rows(to_row(jnp.concatenate([sq[h, i] for h in range(2) for i in range(PARTS)], axis=0)))
        if not last:
            with scope("a_own"):
                columns(t + 1, (OWN,))
                a_phase(t + 1, tiles_of[1] + tiles_of[0], (OWN,))
        for i in range(PARTS):
            with scope("wait_on_a"):
                a_right[i].wait_recv()
            if i < PARTS - DIRECT:
                a_on.append(m_send(LEFT, OPP, 0, i, ON_A + i, right))
            with scope("wait_on_b"):
                b_left[i].wait_recv()
            if i < PARTS - DIRECT:
                b_on.append(m_send(RIGHT, OPP, 1, i, ON_B + i, left))
            swap_piece(LEFT, 0, i)
            swap_piece(RIGHT, 1, i)
        a_on += a_direct
        b_on += b_direct
        if last:
            with scope("wait_rows"):
                for c in rows:
                    c.wait_recv()
            rows_copy = send(row_out, row_in, ROW + 3, SINGLE + 8, partner)
            for i in range(PARTS):
                with scope("wait_bl"):
                    b_right[i].wait_recv()
                swap_piece(LEFT, 1, i)
                with scope("wait_ar"):
                    a_left[i].wait_recv()
                swap_piece(RIGHT, 0, i)
            for i in range(PARTS):
                with scope("wait_oa"):
                    a_on[i].wait_recv()
                swap_piece(OPP, 0, i)
                with scope("wait_ob"):
                    b_on[i].wait_recv()
                swap_piece(OPP, 1, i)
            with scope("wait_d2dr"):
                rows_copy.wait_recv()
            for b in range(4):
                q = lax.rem(chip + SHIFT[b], n_chips)
                logw_out[pl.ds(core * n_chips + q, 1), :] = row_out[b, 0:1, :]
                logw_out[pl.ds((1 - core) * n_chips + q, 1), :] = row_in[b, 0:1, :]
            with scope("wait_d2d"):
                theirs = mean_out.at[pl.ds(pl.multiple_of((1 - core) * half, half), half)]
                pltpu.make_async_remote_copy(
                    src_ref=theirs, dst_ref=theirs, send_sem=send_sem.at[FINAL_OUT], recv_sem=recv_sem.at[FINAL],
                    device_id=partner, device_id_type=MESH,
                ).wait_recv()
    with scope("drain"):
        for c in pending.values():
            c.wait_send()
        wait_group(X_OUT, x_all.at[1])
        wait_sums(sweeps - 1)
        wait_means(sweeps - 1)
        wait_group(FINAL_OUT, mean_out.at[pl.ds(0, half)])


def pass_kernel(mean_in, logw_in, lse_in, mean_out, logw_out, lse_out, sem):
    copies = [
        pltpu.make_async_copy(src, dst, sem.at[i])
        for i, (src, dst) in enumerate(((mean_in, mean_out), (logw_in, logw_out), (lse_in, lse_out)))
    ]
    for c in copies:
        c.start()
    for c in copies:
        c.wait()


def solution(mesh):
    n_pts, n_comp = mesh.shape["pts"], mesh.shape["comp"]
    n_chips = n_pts // CORES

    def per_device(points, means, log_w, inv_temp):
        n_loc, depth = points.shape
        k_loc = means.shape[0]
        kq = k_loc // n_pts
        half = n_chips * kq
        sweeps = inv_temp.shape[0]
        if n_chips != 4 or kq != LANES:
            raise ValueError("unsupported shape")
        f32, bf16 = jnp.float32, jnp.bfloat16
        kernel = functools.partial(
            em_kernel, sweeps, n_loc * n_pts, k_loc * n_comp, n_chips, n_comp
        )
        vmem = pl.BlockSpec(memory_space=pltpu.VMEM)
        hbm = pl.BlockSpec(memory_space=pltpu.HBM)
        V = pltpu.VMEM
        mean, logw, lse = pl.pallas_call(
            kernel,
            out_shape=(
                jax.ShapeDtypeStruct((k_loc, depth), f32),
                jax.ShapeDtypeStruct((n_pts, kq), f32),
                jax.ShapeDtypeStruct((n_loc // LANES, LANES), f32),
            ),
            in_specs=[hbm] * 4,
            out_specs=(vmem, vmem, vmem),
            scratch_shapes=[
                pltpu.SMEM((sweeps,), f32),
                V((n_pts, kq), f32),
                V((2, n_loc, depth), bf16),
                V((depth, 2 * n_loc), bf16),
                V((1, n_loc), f32),
                V((half, 2 * n_loc), f32),
                V((half, 2 * n_loc), bf16),
                V((4, kq, depth), f32),
                V((sweeps, 4, kq, depth), bf16),
                V((sweeps, 4, 8, kq), f32),
                V((4, 2 * n_loc), f32),
                V((4, 2 * n_loc), f32),
                V((4, 2 * n_loc), f32),
                V((sweeps, 2, n_loc), f32),
                V((sweeps, 2, n_loc), f32),
                V((sweeps, 2, n_loc), f32),
                V((sweeps, n_comp - 1, 2, n_loc), f32),
                V((sweeps, 1, n_loc), f32),
                V((sweeps, 1, n_loc), f32),
                V((4, kq, LANES), f32),
                V((half, min(256, n_loc // 2)), f32),
                V((half, min(256, n_loc // 2)), f32),
                V((2, 4, kq, LANES), f32),
                V((sweeps, 8, kq // 2, depth), f32),
                V((sweeps, 6, kq // 2, depth), f32),
                V((sweeps, 2, kq // 2, depth), f32),
                V((sweeps, 4, 8, kq), f32),
                V((sweeps, 3, 8, kq), f32),
                V((4, 8, kq), f32),
                V((4, 8, kq), f32),
                pltpu.SemaphoreType.DMA((SINGLE + 8 + n_comp,)),
                pltpu.SemaphoreType.DMA((ACROSS + sweeps * (n_comp - 1),)),
                pltpu.SemaphoreType.DMA((10,)),
            ],
            compiler_params=pltpu.CompilerParams(
                collective_id=0, has_side_effects=True, vmem_limit_bytes=44 * 1024 * 1024
            ),
            name="em",
        )(*(pltpu.with_memory_space_constraint(v, pltpu.HBM) for v in (inv_temp, points, means, log_w.reshape(n_pts, kq))))
        copies = (mean, logw, lse)
        mean, logw, lse = pl.pallas_call(
            pass_kernel,
            out_shape=tuple(pltpu.HBM(v.shape, f32) for v in copies),
            in_specs=[vmem] * 3,
            out_specs=(hbm,) * 3,
            scratch_shapes=[pltpu.SemaphoreType.DMA((3,))],
            name="results",
        )(*(pltpu.with_memory_space_constraint(v, pltpu.VMEM) for v in copies))
        return mean, logw.reshape(k_loc), lse.reshape(n_loc)

    comp_spec = P(("fit", "comp"))
    return jax.shard_map(
        per_device,
        mesh=mesh,
        in_specs=(P(("fit", "pts"), None), P(("fit", "comp"), None), comp_spec, P()),
        out_specs=(P(("fit", "comp"), None), comp_spec, P(("fit", "pts"))),
        check_vma=False,
    )
```

```python
import contextlib
import functools
import math

import jax
import jax.numpy as jnp
from jax import lax
from jax.experimental import pallas as pl
from jax.experimental.pallas import tpu as pltpu
from jax.sharding import PartitionSpec as P

PRIOR_ALPHA = 1e-3
COUNT_EPS = 1e-6
LOG2E = math.log2(math.e)
LN2 = math.log(2.0)
MESH = pl.DeviceIdType.MESH
scope = contextlib.nullcontext
CORES = 2
PARTS = 2
DIRECT = 0
LANES = 128

OPP, RIGHT, LEFT, OWN = range(4)
SHIFT = {OPP: 2, RIGHT: 1, LEFT: 3, OWN: 0}
ORDER = [(OPP, 0), (OPP, 1), (RIGHT, 1), (LEFT, 0), (RIGHT, 0), (LEFT, 1), (OWN, 0), (OWN, 1)]
PLACE = {piece: i for i, piece in enumerate(ORDER)}

PAIR, SWAP, COUNT, ROW, FINAL, XPART, PIECES = 0, 1, 2, 5, 9, 10, 14
FAR_A, FAR_B, NEAR_A, NEAR_B, SUM_A, SUM_B, OWN_A_RIGHT, OWN_B_RIGHT, OWN_A_LEFT, OWN_B_LEFT, ON_A, ON_B = range(
    PIECES, PIECES + 12 * PARTS, PARTS
)
ACROSS = PIECES + 12 * PARTS
SUMS_RIGHT, SUMS_LEFT, MEANS_RIGHT, MEANS_LEFT, X_OUT, FINAL_OUT, SINGLE = range(7)


def em_kernel(
    sweeps, n_total, k_total, n_chips, n_comp,
    beta_hbm, x_hbm, mean_hbm, logw_hbm,
    mean_out, logw_out, lse_out,
    beta_ref, logw_ref, x_all, xt, x_sq, e_buf, r_buf, mean_f, mean_b, prm, m_st, s_st, factor, pair_out, pair_in, glob_out, glob_in,
    lse_own, lse_oth, cols_c, raw_0, raw_1, n_acc, s_buf, rs_in, acc_out, n_out, n_in, row_out, row_in, send_sem, recv_sem, copy_sem,
):
    raw = (raw_0, raw_1)
    n_loc, depth = x_all.shape[1], x_all.shape[2]
    kq = mean_f.shape[1]
    kh, kp = kq // 2, kq // 2 // PARTS
    half = n_chips * kq

    p = lax.axis_index("pts")
    y = lax.axis_index("comp")
    chip = lax.div(p, CORES)
    core = p - chip * CORES
    partner = {"pts": chip * CORES + 1 - core}

    def x_peer(d):
        return {"pts": lax.rem(chip + d, n_chips) * CORES + core}

    right, left, opposite = x_peer(1), x_peer(n_chips - 1), x_peer(2)
    y_order = sorted(range(1, n_comp), key=lambda d: -min(d, n_comp - d))
    y_peers = [{"comp": lax.rem(y + d, n_comp)} for d in y_order]

    barrier = pltpu.get_barrier_semaphore()
    everyone = [partner, right, left, opposite] + y_peers
    for dev in everyone:
        pl.semaphore_signal(barrier, inc=1, device_id=dev, device_id_type=MESH)

    tr = min(1024, n_loc // 2)
    n_tr = n_loc // tr
    x_rows = [pl.ds(c * tr, tr) for c in range(n_tr)]
    load_x = [pltpu.make_async_copy(x_hbm.at[r], x_all.at[0, r], copy_sem.at[6 + c]) for c, r in enumerate(x_rows)]
    load_x[0].start()
    load_small = [
        pltpu.make_async_copy(logw_hbm, logw_ref, copy_sem.at[4]), pltpu.make_async_copy(beta_hbm, beta_ref, copy_sem.at[5])
    ]
    for c in load_small:
        c.start()
    load_mean = []
    for b in range(4):
        q = lax.rem(chip + SHIFT[b], n_chips)
        c = pltpu.make_async_copy(
            mean_hbm.at[pl.ds(pl.multiple_of(core * half + q * kq, kq), kq)], mean_f.at[b], copy_sem.at[b]
        )
        c.start()
        load_mean.append(c)

    for c in load_x[1:]:
        c.start()

    pending = {}

    def send(src, dst, arrive, depart, dev, when=None):
        c = pltpu.make_async_remote_copy(
            src_ref=src, dst_ref=dst, send_sem=send_sem.at[depart], recv_sem=recv_sem.at[arrive],
            device_id=dev, device_id_type=MESH,
        )
        if depart >= SINGLE:
            if depart in pending:
                pending[depart].wait_send()
            pending[depart] = c
        if when is None:
            c.start()
        else:
            pl.when(when)(c.start)
        return c

    def wait_group(depart, ref):
        pltpu.make_async_remote_copy(
            src_ref=ref, dst_ref=ref, send_sem=send_sem.at[depart], recv_sem=recv_sem.at[PAIR],
            device_id=partner, device_id_type=MESH,
        ).wait_send()

    def wait_sums(t):
        wait_group(SUMS_RIGHT, rs_in.at[t, pl.ds(0, 3)])
        wait_group(SUMS_LEFT, rs_in.at[t, pl.ds(0, 3)])

    def wait_means(t):
        ref = mean_b.at[t + 1, pl.ds(0, 3), pl.ds(0, kh)] if t < sweeps - 1 else mean_out.at[pl.ds(0, 3 * kh)]
        wait_group(MEANS_RIGHT, ref)
        wait_group(MEANS_LEFT, ref)

    eye = lax.broadcasted_iota(jnp.int32, (kq, kq), 0) == lax.broadcasted_iota(jnp.int32, (kq, kq), 1)

    def to_col(row):
        return jnp.sum(jnp.where(eye, jnp.broadcast_to(row, (kq, kq)), 0.0), axis=1, keepdims=True)

    def to_row(col):
        return jnp.sum(jnp.where(eye, jnp.broadcast_to(col, (kq, kq)), 0.0), axis=0, keepdims=True)

    with scope("barrier"):
        pl.semaphore_wait(barrier, len(everyone))
    x_copies = [send(x_hbm.at[r], x_all.at[1, r], XPART + c, X_OUT, partner) for c, r in enumerate(x_rows)]
    with scope("loads"):
        for c in load_small:
            c.wait()
    with scope("meanprep"):
        for b in range(4):
            load_mean[b].wait()
            mf = mean_f[b]
            mean_b[0, b] = mf.astype(jnp.bfloat16)
            q = lax.rem(chip + SHIFT[b], n_chips)
            prm[0, b, 0:1, :] = logw_ref[pl.ds(core * n_chips + q, 1), :]
            prm[0, b, 1:2, :] = to_row(jnp.sum(mf * mf, axis=1, keepdims=True))

    tile = min(512, n_loc // 2)

    def prepare(u):
        h, at = divmod(u * tile, n_loc)
        blk = x_all[h, at:at + tile, :].T
        xt[:, u * tile:(u + 1) * tile] = blk
        if h == 0:
            f = blk.astype(jnp.float32)
            x_sq[:, at:at + tile] = jnp.sum(f * f, axis=0, keepdims=True)

    def columns(t, blocks):
        for b in blocks:
            row = (prm[t, b, 0:1, :] - beta_ref[t] * prm[t, b, 1:2, :]) * LOG2E
            cols_c[b] = jnp.broadcast_to(to_col(row), (kq, LANES))

    def a_phase(t, tiles, blocks, ahead=None):
        slope = beta_ref[t] * (2.0 * LOG2E)
        lo, nb = blocks[0], len(blocks)
        means = mean_b.at[t, lo:lo + nb]

        def product(u):
            cols = slice(tiles[u] * tile, (tiles[u] + 1) * tile)
            raw[u % 2][0:nb * kq] = jnp.dot(
                means[...].reshape(nb * kq, depth), xt[:, cols], preferred_element_type=jnp.float32
            )

        if ahead is not None:
            ahead(tiles[0])
            ahead(tiles[1])
        product(0)
        for u in range(len(tiles)):
            if u + 1 < len(tiles):
                product(u + 1)
            if ahead is not None and u + 2 < len(tiles):
                ahead(tiles[u + 2])
            for v in range(tile // LANES):
                at = tiles[u] * tile + v * LANES
                cols = slice(at, at + LANES)
                for i, b in enumerate(blocks):
                    a = raw[u % 2][i * kq:(i + 1) * kq, v * LANES:(v + 1) * LANES]
                    logit = a * slope + cols_c[b]
                    m = jnp.max(logit, axis=0, keepdims=True)
                    e = jnp.exp2(logit - m)
                    for half_b in range(2):
                        at_row = PLACE[b, half_b] * kh
                        e_buf[at_row:at_row + kh, cols] = e[half_b * kh:(half_b + 1) * kh]
                    m_st[b:b + 1, cols] = m
                    s_st[b:b + 1, cols] = jnp.sum(e, axis=0, keepdims=True)

    per_half = n_loc // tile
    tiles_of = [list(range(per_half)), list(range(per_half, 2 * per_half))]

    def local_pair(h):
        cols = pl.ds(h * n_loc, n_loc)
        ms = [m_st[b:b + 1, cols] for b in range(4)]
        m = jnp.maximum(jnp.maximum(ms[0], ms[1]), jnp.maximum(ms[2], ms[3]))
        s = sum(s_st[b:b + 1, cols] * jnp.exp2(ms[b] - m) for b in range(4))
        return m, s

    def r_phase(h, group, lse):
        half_cols = slice(h * n_loc, (h + 1) * n_loc)
        if group == 0:
            factor[:, half_cols] = jnp.exp2(m_st[:, half_cols] - lse[...])
        places = range(4 * group, 4 * group + 4)
        accs = [jnp.zeros((kh, LANES), jnp.float32) for _ in places]
        for c in range(n_loc // LANES):
            cols = slice(h * n_loc + c * LANES, h * n_loc + (c + 1) * LANES)
            for i, place in enumerate(places):
                b = ORDER[place][0]
                r = e_buf[place * kh:(place + 1) * kh, cols] * factor[b:b + 1, cols]
                r_buf[place * kh:(place + 1) * kh, cols] = r.astype(jnp.bfloat16)
                accs[i] = accs[i] + r
        for i, place in enumerate(places):
            n_acc[h, place] = accs[i]

    def stats(h, group):
        rows = slice(4 * group * kh, 4 * (group + 1) * kh)
        out = jnp.dot(
            r_buf[rows, h * n_loc:(h + 1) * n_loc], x_all[h], preferred_element_type=jnp.float32
        ).reshape(4, kh, depth)
        if h == 0:
            s_buf[t, 4 * group:4 * group + 4] = out
        else:
            s_buf[t, 4 * group:4 * group + 4] += out

    for t in range(sweeps):
        last = t == sweeps - 1
        if t == 0:
            columns(0, range(4))
            with scope("loadx"):
                for c in load_x:
                    c.wait()
            with scope("a00"):
                a_phase(t, tiles_of[0], range(4), prepare)
            for g in range(2):
                with scope("xwait"):
                    for c in x_copies[g * n_tr // 2:(g + 1) * n_tr // 2]:
                        c.wait_recv()
                with scope("a01"):
                    a_phase(t, tiles_of[1][g * per_half // 2:(g + 1) * per_half // 2], range(4), prepare)
        else:
            with scope("wait_near"):
                for c in b_right + a_left + rows[:2]:
                    c.wait_recv()
            with scope("a_right"):
                columns(t, (RIGHT, LEFT))
                a_phase(t, tiles_of[1] + tiles_of[0], (RIGHT, LEFT))
            with scope("wait_opp"):
                for c in a_on + b_on + rows[2:]:
                    c.wait_recv()
            with scope("a_opp1"):
                columns(t, (OPP,))
                a_phase(t, tiles_of[1], (OPP,))
        m, s = local_pair(1)
        pair_out[t, 0:1, :] = m
        pair_out[t, 1:2, :] = s
        pair = send(pair_out.at[t], pair_in.at[t], PAIR, SINGLE, partner)
        if t > 0:
            with scope("a_opp0"):
                a_phase(t, tiles_of[0], (OPP,))
        m, s = local_pair(0)
        with scope("wait_pair"):
            pair.wait_recv()
        m1, s1 = pair_in[t, 0:1, :], pair_in[t, 1:2, :]
        top = jnp.maximum(m, m1)
        s = s * jnp.exp2(m - top) + s1 * jnp.exp2(m1 - top)
        glob_out[t, 0:1, :] = top
        glob_out[t, 1:2, :] = s
        across = [
            send(glob_out.at[t], glob_in.at[t, d], ACROSS + t * (n_comp - 1) + d, SINGLE + 9 + d, y_peers[d])
            for d in range(n_comp - 1)
        ]
        tops, sums = [top], [s]
        for d in reversed(range(n_comp - 1)):
            with scope("wait_y"):
                across[d].wait_recv()
            tops.append(glob_in[t, d, 0:1, :])
            sums.append(glob_in[t, d, 1:2, :])
        top = functools.reduce(jnp.maximum, tops)
        total = sum(v * jnp.exp2(w - top) for v, w in zip(sums, tops))
        lse2 = top + jnp.log(total) * LOG2E
        lse_own[t] = lse2
        swap = send(lse_own.at[t], lse_oth.at[t], SWAP, SINGLE + 1, partner)
        if last:
            lse = lse2 * LN2 - beta_ref[t] * x_sq[...]
            for i in range(n_loc // LANES):
                lse_out[i:i + 1, :] = lse[:, i * LANES:(i + 1) * LANES]

        own_r, oth_r = lse_own.at[t], lse_oth.at[t]
        with scope("r_own_a"):
            r_phase(0, 0, own_r)
        with scope("stats0"):
            stats(0, 0)
        with scope("wait_swap"):
            swap.wait_recv()
        with scope("r_oth_a"):
            r_phase(1, 0, oth_r)
        with scope("stats1"):
            stats(1, 0)

        parts = [pl.ds(i * kp, kp) for i in range(PARTS)]

        def s_piece(b, half_b, i):
            return s_buf.at[t, PLACE[b, half_b], parts[i]]

        def in_piece(slot, i):
            return rs_in.at[t, slot, parts[i]]

        def near_b_send(i, when=None):
            return send(s_piece(RIGHT, 1, i), in_piece(2, i), NEAR_B + i, SUMS_RIGHT, right, when)

        def near_a_send(i, when=None):
            return send(s_piece(LEFT, 0, i), in_piece(3, i), NEAR_A + i, SUMS_LEFT, left, when)

        def first_sends(when):
            a, b = [], []
            for i in range(PARTS):
                a.append(send(s_piece(OPP, 0, i), in_piece(0, i), FAR_A + i, SUMS_RIGHT, right, when))
                b.append(send(s_piece(OPP, 1, i), in_piece(1, i), FAR_B + i, SUMS_LEFT, left, when))
            return a, b, [near_b_send(i, when) for i in range(2)], [near_a_send(i, when) for i in range(2)]

        if t > 0:
            wait_sums(t - 1)
        far_a, far_b, near_b, near_a = first_sends(core == 0)
        with scope("r_23"):
            r_phase(0, 1, own_r)
            r_phase(1, 1, oth_r)
        counts = []
        for b in range(4):
            by_lane = [n_acc[0, PLACE[b, half_b]] + n_acc[1, PLACE[b, half_b]] for half_b in range(2)]
            row = to_row(jnp.sum(jnp.concatenate(by_lane, axis=0), axis=1, keepdims=True))
            n_out[t, b, 0:1, :] = row
            counts.append(row)
        n_copies = [
            send(n_out.at[t, b], n_in.at[t, d], COUNT + d, SINGLE + 2 + d, dev)
            for d, (b, dev) in enumerate(((OPP, opposite), (RIGHT, right), (LEFT, left)))
        ]
        with scope("stats2"):
            stats(0, 1)
            stats(1, 1)
        first_sends(core == 1)
        sum_a, sum_b = [], []
        for i in range(PARTS):
            with scope("wait_far_a"):
                far_a[i].wait_recv()
            acc_out[t, 0, parts[i]] = s_buf[t, PLACE[RIGHT, 0], parts[i]] + rs_in[t, 0, parts[i]]
            sum_a.append(send(acc_out.at[t, 0, parts[i]], in_piece(4, i), SUM_A + i, SUMS_RIGHT, right))
            if i + 2 < PARTS:
                near_b.append(near_b_send(i + 2))
            with scope("wait_far_b"):
                far_b[i].wait_recv()
            acc_out[t, 1, parts[i]] = s_buf[t, PLACE[LEFT, 1], parts[i]] + rs_in[t, 1, parts[i]]
            sum_b.append(send(acc_out.at[t, 1, parts[i]], in_piece(5, i), SUM_B + i, SUMS_LEFT, left))
            if i + 2 < PARTS:
                near_a.append(near_a_send(i + 2))

        n_row = counts[OWN]
        for d in range(3):
            with scope("wait_n"):
                n_copies[d].wait_recv()
            n_row = n_row + n_in[t, d, 0:1, :]
        n_col = to_col(n_row) + COUNT_EPS
        logw = jnp.log((n_row + PRIOR_ALPHA) / (n_total + k_total * PRIOR_ALPHA))

        def m_piece(b, half_b, i):
            at = half_b * kh + i * kp
            if not last:
                return mean_b.at[t + 1, b, pl.ds(at, kp)]
            q = lax.rem(chip + SHIFT[b], n_chips)
            return mean_out.at[pl.ds(pl.multiple_of(core * half + q * kq + at, kp), kp)]

        def m_send(b, there, half_b, i, arrive, dev):
            depart = MEANS_LEFT if arrive >= OWN_A_LEFT and not ON_A <= arrive < ON_B else MEANS_RIGHT
            return send(m_piece(b, half_b, i), m_piece(b if last else there, half_b, i), arrive, depart, dev)

        def swap_piece(b, half_b, i):
            if last:
                send(m_piece(b, half_b, i), m_piece(b, half_b, i), FINAL, FINAL_OUT, partner)

        rows = []

        def send_rows(mean_sq=None):
            own_row, to_rows = (row_out.at[OWN], row_out) if last else (prm.at[t + 1, OWN], prm.at[t + 1])
            own_row[0:1, :] = logw
            if mean_sq is not None:
                own_row[1:2, :] = mean_sq
            for d, (b, dev) in enumerate(((LEFT, right), (RIGHT, left), (OPP, opposite))):
                rows.append(send(own_row, to_rows.at[b], ROW + d, SINGLE + 5 + d, dev))

        if t > 0:
            wait_means(t - 1)
        if last:
            send_rows()
        sq = {}
        a_right, b_right, a_left, b_left, a_on, b_on, a_direct, b_direct = ([] for _ in range(8))
        for i in range(PARTS):
            for half_b, far, near, slots in ((0, sum_a, near_a, (3, 4)), (1, sum_b, near_b, (2, 5))):
                with scope("wait_sum"):
                    near[i].wait_recv()
                    far[i].wait_recv()
                at = half_b * kh + i * kp
                mean = (
                    s_buf[t, PLACE[OWN, half_b], parts[i]] + rs_in[t, slots[0], parts[i]] + rs_in[t, slots[1], parts[i]]
                ) / n_col[at:at + kp]
                m_piece(OWN, half_b, i)[...] = mean if last else mean.astype(jnp.bfloat16)
                sq[half_b, i] = jnp.sum(mean * mean, axis=1, keepdims=True)
                if half_b == 0:
                    a_right.append(m_send(OWN, LEFT, 0, i, OWN_A_RIGHT + i, right))
                else:
                    b_left.append(m_send(OWN, RIGHT, 1, i, OWN_B_LEFT + i, left))
            b_right.append(m_send(OWN, LEFT, 1, i, OWN_B_RIGHT + i, right))
            a_left.append(m_send(OWN, RIGHT, 0, i, OWN_A_LEFT + i, left))
            if i >= PARTS - DIRECT:
                a_direct.append(m_send(OWN, OPP, 0, i, ON_A + i, opposite))
                b_direct.append(m_send(OWN, OPP, 1, i, ON_B + i, opposite))
            swap_piece(OWN, 0, i)
            swap_piece(OWN, 1, i)

        if not last:
            send_rows(to_row(jnp.concatenate([sq[h, i] for h in range(2) for i in range(PARTS)], axis=0)))
        if not last:
            with scope("a_own"):
                columns(t + 1, (OWN,))
                a_phase(t + 1, tiles_of[1] + tiles_of[0], (OWN,))
        for i in range(PARTS):
            with scope("wait_on_a"):
                a_right[i].wait_recv()
            if i < PARTS - DIRECT:
                a_on.append(m_send(LEFT, OPP, 0, i, ON_A + i, right))
            with scope("wait_on_b"):
                b_left[i].wait_recv()
            if i < PARTS - DIRECT:
                b_on.append(m_send(RIGHT, OPP, 1, i, ON_B + i, left))
            swap_piece(LEFT, 0, i)
            swap_piece(RIGHT, 1, i)
        a_on += a_direct
        b_on += b_direct
        if last:
            with scope("wait_rows"):
                for c in rows:
                    c.wait_recv()
            rows_copy = send(row_out, row_in, ROW + 3, SINGLE + 8, partner)
            for i in range(PARTS):
                with scope("wait_bl"):
                    b_right[i].wait_recv()
                swap_piece(LEFT, 1, i)
                with scope("wait_ar"):
                    a_left[i].wait_recv()
                swap_piece(RIGHT, 0, i)
            for i in range(PARTS):
                with scope("wait_oa"):
                    a_on[i].wait_recv()
                swap_piece(OPP, 0, i)
                with scope("wait_ob"):
                    b_on[i].wait_recv()
                swap_piece(OPP, 1, i)
            with scope("wait_d2dr"):
                rows_copy.wait_recv()
            for b in range(4):
                q = lax.rem(chip + SHIFT[b], n_chips)
                logw_out[pl.ds(core * n_chips + q, 1), :] = row_out[b, 0:1, :]
                logw_out[pl.ds((1 - core) * n_chips + q, 1), :] = row_in[b, 0:1, :]
            with scope("wait_d2d"):
                theirs = mean_out.at[pl.ds(pl.multiple_of((1 - core) * half, half), half)]
                pltpu.make_async_remote_copy(
                    src_ref=theirs, dst_ref=theirs, send_sem=send_sem.at[FINAL_OUT], recv_sem=recv_sem.at[FINAL],
                    device_id=partner, device_id_type=MESH,
                ).wait_recv()
    with scope("drain"):
        for c in pending.values():
            c.wait_send()
        wait_group(X_OUT, x_all.at[1])
        wait_sums(sweeps - 1)
        wait_means(sweeps - 1)
        wait_group(FINAL_OUT, mean_out.at[pl.ds(0, half)])


def pass_kernel(mean_in, logw_in, lse_in, mean_out, logw_out, lse_out, sem):
    copies = [
        pltpu.make_async_copy(src, dst, sem.at[i])
        for i, (src, dst) in enumerate(((mean_in, mean_out), (logw_in, logw_out), (lse_in, lse_out)))
    ]
    for c in copies:
        c.start()
    for c in copies:
        c.wait()


def solution(mesh):
    n_pts, n_comp = mesh.shape["pts"], mesh.shape["comp"]
    n_chips = n_pts // CORES

    def per_device(points, means, log_w, inv_temp):
        n_loc, depth = points.shape
        k_loc = means.shape[0]
        kq = k_loc // n_pts
        half = n_chips * kq
        sweeps = inv_temp.shape[0]
        if n_chips != 4 or kq != LANES:
            raise ValueError("unsupported shape")
        f32, bf16 = jnp.float32, jnp.bfloat16
        kernel = functools.partial(
            em_kernel, sweeps, n_loc * n_pts, k_loc * n_comp, n_chips, n_comp
        )
        vmem = pl.BlockSpec(memory_space=pltpu.VMEM)
        hbm = pl.BlockSpec(memory_space=pltpu.HBM)
        V = pltpu.VMEM
        mean, logw, lse = pl.pallas_call(
            kernel,
            out_shape=(
                jax.ShapeDtypeStruct((k_loc, depth), f32),
                jax.ShapeDtypeStruct((n_pts, kq), f32),
                jax.ShapeDtypeStruct((n_loc // LANES, LANES), f32),
            ),
            in_specs=[hbm] * 4,
            out_specs=(vmem, vmem, vmem),
            scratch_shapes=[
                pltpu.SMEM((sweeps,), f32),
                V((n_pts, kq), f32),
                V((2, n_loc, depth), bf16),
                V((depth, 2 * n_loc), bf16),
                V((1, n_loc), f32),
                V((half, 2 * n_loc), f32),
                V((half, 2 * n_loc), bf16),
                V((4, kq, depth), f32),
                V((sweeps, 4, kq, depth), bf16),
                V((sweeps, 4, 8, kq), f32),
                V((4, 2 * n_loc), f32),
                V((4, 2 * n_loc), f32),
                V((4, 2 * n_loc), f32),
                V((sweeps, 2, n_loc), f32),
                V((sweeps, 2, n_loc), f32),
                V((sweeps, 2, n_loc), f32),
                V((sweeps, n_comp - 1, 2, n_loc), f32),
                V((sweeps, 1, n_loc), f32),
                V((sweeps, 1, n_loc), f32),
                V((4, kq, LANES), f32),
                V((half, min(512, n_loc // 2)), f32),
                V((half, min(512, n_loc // 2)), f32),
                V((2, 8, kq // 2, LANES), f32),
                V((sweeps, 8, kq // 2, depth), f32),
                V((sweeps, 6, kq // 2, depth), f32),
                V((sweeps, 2, kq // 2, depth), f32),
                V((sweeps, 4, 8, kq), f32),
                V((sweeps, 3, 8, kq), f32),
                V((4, 8, kq), f32),
                V((4, 8, kq), f32),
                pltpu.SemaphoreType.DMA((SINGLE + 8 + n_comp,)),
                pltpu.SemaphoreType.DMA((ACROSS + sweeps * (n_comp - 1),)),
                pltpu.SemaphoreType.DMA((10,)),
            ],
            compiler_params=pltpu.CompilerParams(
                collective_id=0, has_side_effects=True, vmem_limit_bytes=44 * 1024 * 1024
            ),
            name="em",
        )(*(pltpu.with_memory_space_constraint(v, pltpu.HBM) for v in (inv_temp, points, means, log_w.reshape(n_pts, kq))))
        copies = (mean, logw, lse)
        mean, logw, lse = pl.pallas_call(
            pass_kernel,
            out_shape=tuple(pltpu.HBM(v.shape, f32) for v in copies),
            in_specs=[vmem] * 3,
            out_specs=(hbm,) * 3,
            scratch_shapes=[pltpu.SemaphoreType.DMA((3,))],
            name="results",
        )(*(pltpu.with_memory_space_constraint(v, pltpu.VMEM) for v in copies))
        return mean, logw.reshape(k_loc), lse.reshape(n_loc)

    comp_spec = P(("fit", "comp"))
    return jax.shard_map(
        per_device,
        mesh=mesh,
        in_specs=(P(("fit", "pts"), None), P(("fit", "comp"), None), comp_spec, P()),
        out_specs=(P(("fit", "comp"), None), comp_spec, P(("fit", "pts"))),
        check_vma=False,
    )
```
